32 devices in a mesh: tp: 4 (over z), dp: 8 (over y, x, core).
Axes of the slice: x: 2, y: 2, z: 4, core: 2. Of those that a mesh axis runs over, the one named last changes fastest.
Arguments:
- hidden: bfloat16 [8192, 576], P('dp')
- norm_w: bfloat16 [576], replicated
- emb_table: bfloat16 [49152, 576], P('tp')
- teacher: bfloat16 [8192, 49152], P('dp', 'tp')
- loss_mask: int32 [8192], P('dp')
Outputs:
- output 1: float32 [], replicated
- output 2: bfloat16 [8192, 576], P('dp')
- output 3: float32 [49152, 576], P('tp', 'dp')
- output 4: float32 [576], replicated
All inputs are finite; a program needn't handle non-finite values.
Results may differ from the reference program's by a relative error of at most 0.001.
Values sent between devices are 32-bit elements.
A program may use at most 1 GiB of HBM per device.

```python
import jax
import jax.numpy as jnp
from jax import lax

MODEL_DIM = 576
VOCAB_SIZE = 49152
TOK_DEV = 1024
DP_SHARDS = 8
TOKENS = TOK_DEV * DP_SHARDS
SOFT_CAP = 30.0
NORM_EPS = 1e-6


def setup_inputs(seed: int = 0) -> dict:
    base_key = jax.random.key(seed)
    key_list = jax.random.split(base_key, 6)
    hidden = jax.random.normal(key_list[0], (TOKENS, MODEL_DIM), jnp.float32)
    norm_w = 0.5 * jax.random.normal(key_list[1], (MODEL_DIM,), jnp.float32)
    mean_dir = jax.random.normal(key_list[2], (MODEL_DIM,), jnp.float32)
    emb_noise = jax.random.normal(key_list[3], (VOCAB_SIZE, MODEL_DIM), jnp.float32)
    emb_table = (18.0 * mean_dir[None, :] + 1.5 * emb_noise) * (MODEL_DIM ** -0.5)
    teacher = 2.0 * jax.random.normal(key_list[4], (TOKENS, VOCAB_SIZE), jnp.float32)
    lengths = jax.random.randint(key_list[5], (DP_SHARDS,), 1, TOK_DEV + 1)
    lengths = jnp.where(jnp.arange(DP_SHARDS) == 0, TOK_DEV, lengths)
    loss_mask = (jnp.arange(TOK_DEV)[None, :] < lengths[:, None]).astype(jnp.int32)
    return {'hidden': hidden.astype(jnp.bfloat16), 'norm_w': norm_w.astype(jnp.bfloat16), 'emb_table': emb_table.astype(jnp.bfloat16), 'teacher': teacher.astype(jnp.bfloat16), 'loss_mask': loss_mask.reshape(TOKENS)}


def rms_norm(hid_f32, scale_f32):
    inv_rms = lax.rsqrt(jnp.mean(hid_f32 * hid_f32, axis=-1, keepdims=True) + NORM_EPS)
    return hid_f32 * inv_rms * (1.0 + scale_f32)


def reference(hidden, norm_w, emb_table, teacher, loss_mask):
    mask_f32 = loss_mask.astype(jnp.float32)
    weights = mask_f32 / jnp.sum(mask_f32)
    scale_f32 = norm_w.astype(jnp.float32)

    def block_step(acc_state, blk_inputs):
        emb_acc, scale_acc = acc_state
        hid_blk, teach_blk, weight_blk = blk_inputs
        normed_f32, norm_pull = jax.vjp(rms_norm, hid_blk.astype(jnp.float32), scale_f32)
        normed = normed_f32.astype(jnp.bfloat16)
        raw_logit = jnp.dot(normed, emb_table.T, preferred_element_type=jnp.float32)
        tanh_val = jnp.tanh(raw_logit / SOFT_CAP)
        capped = SOFT_CAP * tanh_val
        log_stu = jax.nn.log_softmax(capped, axis=-1)
        log_tea = jax.nn.log_softmax(teach_blk.astype(jnp.float32), axis=-1)
        prob_tea = jnp.exp(log_tea)
        kl_tok = jnp.sum(prob_tea * (log_tea - log_stu), axis=-1)
        loss_part = jnp.sum(weight_blk * kl_tok)
        d_raw = ((jnp.exp(log_stu) - prob_tea) * weight_blk[:, None] * (1.0 - tanh_val * tanh_val)).astype(jnp.bfloat16)
        grad_normed = jnp.dot(d_raw, emb_table, preferred_element_type=jnp.float32)
        emb_acc = emb_acc + jnp.dot(d_raw.T, normed, preferred_element_type=jnp.float32)
        grad_hid, grad_scale = norm_pull(grad_normed)
        return (emb_acc, scale_acc + grad_scale), (loss_part, grad_hid.astype(jnp.bfloat16))

    blocks_in = (hidden.reshape(DP_SHARDS, TOK_DEV, MODEL_DIM), teacher.reshape(DP_SHARDS, TOK_DEV, VOCAB_SIZE), weights.reshape(DP_SHARDS, TOK_DEV))
    start_acc = (jnp.zeros((VOCAB_SIZE, MODEL_DIM), jnp.float32), jnp.zeros((MODEL_DIM,), jnp.float32))
    final_acc, per_block = lax.scan(block_step, start_acc, blocks_in)
    d_emb, d_norm_w = final_acc
    loss_parts, grad_hid = per_block
    return jnp.sum(loss_parts), grad_hid.reshape(TOKENS, MODEL_DIM), d_emb, d_norm_w
```

```python
import jax
import jax.numpy as jnp
from jax import lax
from jax.experimental import pallas as pl
from jax.experimental.pallas import tpu as pltpu
from jax.sharding import PartitionSpec as P

SOFT_CAP = 30.0
NORM_EPS = 1e-6
LOG2E = 1.4426950408889634
LN2 = 0.6931471805599453
CAP2 = SOFT_CAP * LOG2E
D = 576
GRP = 72
TOK = 1024
VLOC = 12288
CW = 512
HALF = CW // 2
NCH = VLOC // CW
RG = 32
F32 = jnp.float32
BF16 = jnp.bfloat16
NT = (((1,), (1,)), ((), ()))


def lane_tiles(arr):
    return [arr[:, k * 128:(k + 1) * 128] for k in range(arr.shape[1] // 128)]


def tree(op, parts):
    while len(parts) > 1:
        parts = [op(parts[k], parts[k + 1]) if k + 1 < len(parts) else parts[k] for k in range(0, len(parts), 2)]
    return parts[0]


def stats_kernel(hid_ref, w_ref, emb_ref, tea_ref, th_ref, gt_ref, st_ref, g_scr, s_acc, m_acc, t_acc):
    step = pl.program_id(0)

    @pl.when(step == 0)
    def _():
        x = hid_ref[...].astype(F32)
        inv = lax.rsqrt(jnp.mean(x * x, axis=0, keepdims=True) + NORM_EPS)
        gn = x * inv * (1.0 + w_ref[...])
        gt_ref[...] = gn.astype(BF16)
        g_scr[...] = jnp.transpose(gn).astype(BF16)
        s_acc[...] = jnp.zeros_like(s_acc)
        t_acc[...] = jnp.zeros_like(t_acc)
        m_acc[...] = jnp.full_like(m_acc, -jnp.inf)

    tb = 256
    for blk in range(TOK // tb):
        raw = jnp.dot(g_scr[blk * tb:(blk + 1) * tb, :], emb_ref[...], preferred_element_type=F32)
        for sub in range(tb // RG):
            rows = slice(blk * tb + sub * RG, blk * tb + (sub + 1) * RG)
            th = jnp.tanh(raw[sub * RG:(sub + 1) * RG, :] * (1.0 / SOFT_CAP))
            th_ref[rows, :] = th
            s_acc[rows, :] += tree(jnp.add, lane_tiles(jnp.exp2(th * CAP2 - CAP2)))
            tea = lane_tiles(tea_ref[rows, :].astype(F32))
            old = m_acc[rows, :]
            new = jnp.maximum(old, tree(jnp.maximum, tea))
            m_acc[rows, :] = new
            t_acc[rows, :] = t_acc[rows, :] * jnp.exp2((old - new) * LOG2E) + tree(
                jnp.add, [jnp.exp2((part - new) * LOG2E) for part in tea])

    @pl.when(step == NCH - 1)
    def _():
        s_row = jnp.sum(jnp.transpose(s_acc[...]), axis=0, keepdims=True)
        m_t = jnp.transpose(m_acc[...])
        m_row = jnp.max(m_t, axis=0, keepdims=True)
        t_row = jnp.sum(jnp.transpose(t_acc[...]) * jnp.exp2((m_t - m_row) * LOG2E), axis=0, keepdims=True)
        st_ref[...] = jnp.concatenate([s_row, m_row, t_row, jnp.zeros((5, TOK), F32)], axis=0)


def first_pass(hid_t, w_col, emb_t, teach):
    return pl.pallas_call(
        stats_kernel,
        grid=(NCH,),
        out_shape=(
            jax.ShapeDtypeStruct((TOK, VLOC), F32),
            jax.ShapeDtypeStruct((D, TOK), BF16),
            jax.ShapeDtypeStruct((8, TOK), F32),
        ),
        in_specs=[
            pl.BlockSpec((D, TOK), lambda i: (0, 0)),
            pl.BlockSpec((D, 1), lambda i: (0, 0)),
            pl.BlockSpec((D, CW), lambda i: (0, i)),
            pl.BlockSpec((TOK, CW), lambda i: (0, i)),
        ],
        out_specs=(
            pl.BlockSpec((TOK, CW), lambda i: (0, i)),
            pl.BlockSpec((D, TOK), lambda i: (0, 0)),
            pl.BlockSpec((8, TOK), lambda i: (0, 0)),
        ),
        scratch_shapes=[pltpu.VMEM((TOK, D), BF16)] + [pltpu.VMEM((TOK, 128), F32)] * 3,
        compiler_params=pltpu.CompilerParams(
            dimension_semantics=("arbitrary",), vmem_limit_bytes=48 * 1024 * 1024),
        cost_estimate=pl.CostEstimate(
            flops=2 * TOK * VLOC * D, bytes_accessed=90_000_000, transcendentals=3 * TOK * VLOC),
    )(hid_t, w_col, emb_t, teach)


def grad_kernel(th_hbm, tea_hbm, emb_hbm, gt_ref, hid_ref, w_ref, st_ref, mask_ref,
                de_ref, dh_ref, dw_ref, loss_ref,
                th_buf, tea_buf, emb_buf, dr0, dr1, pp0, pp1, r1, r2a, r2b, r3a, r3b,
                dg_ref, ar_in, dh_f, st_in, cnt_in, cnt_own, wgt, l2s, mtx, l2t, kl_acc,
                in_sem, st_send, st_recv, cnt_send, cnt_recv,
                s1_send, s1_recv, s2_send, s2_recv, s3_send, s3_recv,
                ar_send, ar_recv, bc_send, bc_recv):
    z = lax.axis_index('tp')
    d = lax.axis_index('dp')
    core = d % 2
    xx = (d // 2) % 2
    yy = d // 4
    partner = d + 1 - 2 * core
    xnbr = d + 2 - 4 * xx
    ynbr = d + 4 - 8 * yy

    def fetch(i):
        cols = pl.ds(pl.multiple_of(i * CW, CW), CW)
        three = i % 3
        four = i % 4
        return (
            pltpu.make_async_copy(th_hbm.at[:, cols], th_buf.at[three], in_sem.at[0, three]),
            pltpu.make_async_copy(tea_hbm.at[:, cols], tea_buf.at[three], in_sem.at[1, three]),
            pltpu.make_async_copy(emb_hbm.at[:, cols], emb_buf.at[four], in_sem.at[2, four]),
        )

    def start_fetch(i):
        for cp in fetch(i):
            cp.start()

    start_fetch(0)
    start_fetch(1)

    barrier = pltpu.get_barrier_semaphore()
    for k in range(1, 4):
        pl.semaphore_signal(barrier, inc=1, device_id={'tp': (z + k) % 4})
    for k in range(1, 8):
        pl.semaphore_signal(barrier, inc=1, device_id={'dp': (d + k) % 8})
    cnt_own[...] = jnp.full((8, 128), jnp.sum(mask_ref[...]), F32)
    pl.semaphore_wait(barrier, 10)

    def st_copy(k):
        return pltpu.make_async_remote_copy(
            src_ref=st_ref, dst_ref=st_in.at[k], send_sem=st_send.at[k], recv_sem=st_recv.at[k],
            device_id={'tp': (z + k) % 4})

    def cnt_copy(k):
        return pltpu.make_async_remote_copy(
            src_ref=cnt_own, dst_ref=cnt_in.at[k], send_sem=cnt_send.at[k], recv_sem=cnt_recv.at[k],
            device_id={'dp': (d + k) % 8})

    for k in range(1, 4):
        st_copy(k).start()
    for k in range(1, 8):
        cnt_copy(k).start()
    dg_ref[...] = jnp.zeros_like(dg_ref)
    kl_acc[...] = jnp.zeros_like(kl_acc)
    dw_ref[...] = jnp.zeros_like(dw_ref)
    for k in range(1, 4):
        st_copy(k).wait_recv()
    for k in range(1, 8):
        cnt_copy(k).wait_recv()

    stats = [st_ref[...]] + [st_in[k] for k in range(1, 4)]
    s_tot = tree(jnp.add, [st[0:1, :] for st in stats])
    m_tot = tree(jnp.maximum, [st[1:2, :] for st in stats])
    t_tot = tree(jnp.add, [st[2:3, :] * jnp.exp2((st[1:2, :] - m_tot) * LOG2E) for st in stats])
    count = cnt_own[0:1, :]
    for k in range(1, 8):
        count = count + cnt_in[k][0:1, :]
    w_row = mask_ref[...] / jnp.concatenate([count] * (TOK // 128), axis=1)
    l2s_row = jnp.log2(s_tot) + CAP2
    l2t_row = jnp.log2(t_tot)

    def to_rows(row):
        return jnp.transpose(jnp.broadcast_to(row, (128, TOK)))

    wgt[...] = to_rows(w_row)
    l2s[...] = to_rows(l2s_row)
    mtx[...] = to_rows(m_tot)
    l2t[...] = to_rows(l2t_row)
    lse_part = w_row * ((l2s_row - l2t_row) * LN2 - m_tot)
    lse_sum = jnp.where(z == 0, jnp.sum(lse_part), 0.0)

    def elementwise(i, dr_ref, lo, hi):
        slot = i % 3
        for sub in range(lo, hi):
            rows = slice(sub * RG, (sub + 1) * RG)
            w_b, ls_b, m_b, lt_b = wgt[rows, :], l2s[rows, :], mtx[rows, :], l2t[rows, :]
            kl = []
            for q in range(CW // 128):
                cols = slice(q * 128, (q + 1) * 128)
                th = th_buf[slot, rows, cols]
                tea = tea_buf[slot, rows, cols].astype(F32)
                p_s = jnp.exp2(th * CAP2 - ls_b)
                p_t = jnp.exp2((tea - m_b) * LOG2E - lt_b)
                kl.append(p_t * (tea - SOFT_CAP * th))
                dr_ref[rows, cols] = ((p_s - p_t) * w_b * (1.0 - th * th)).astype(BF16)
            kl_acc[rows, :] += tree(jnp.add, kl)

    def emb_piece(dr_ref, pp_ref, k):
        part = jnp.dot(gt_ref[...], dr_ref[:, k * HALF:(k + 1) * HALF], preferred_element_type=F32)
        for grp in range(8):
            pp_ref[grp % 2, grp // 4, (grp // 2) % 2, :, k * HALF:(k + 1) * HALF] = part[grp * GRP:(grp + 1) * GRP, :]

    def hid_piece(i, dr_ref, k):
        cols = slice(k * 256, (k + 1) * 256)
        dg_ref[:, cols] += lax.dot_general(emb_buf[i % 4], dr_ref[cols, :], NT, preferred_element_type=F32)

    def s1_copy(c, pp_ref):
        return pltpu.make_async_remote_copy(
            src_ref=pp_ref.at[1 - core], dst_ref=r1.at[c], send_sem=s1_send.at[c], recv_sem=s1_recv.at[c],
            device_id={'dp': partner})

    def s2_copies(c):
        return (
            pltpu.make_async_remote_copy(
                src_ref=r1.at[c, :, 1 - xx, :, pl.ds(0, HALF)], dst_ref=r2a.at[c],
                send_sem=s2_send.at[0, c], recv_sem=s2_recv.at[0, c], device_id={'dp': xnbr}),
            pltpu.make_async_remote_copy(
                src_ref=r1.at[c, 1 - yy, :, :, pl.ds(HALF, HALF)], dst_ref=r2b.at[c],
                send_sem=s2_send.at[1, c], recv_sem=s2_recv.at[1, c], device_id={'dp': ynbr}),
        )

    def s3_copies(c):
        return (
            pltpu.make_async_remote_copy(
                src_ref=r2a.at[c, 1 - yy], dst_ref=r3a.at[c],
                send_sem=s3_send.at[0, c], recv_sem=s3_recv.at[0, c], device_id={'dp': ynbr}),
            pltpu.make_async_remote_copy(
                src_ref=r2b.at[c, 1 - xx], dst_ref=r3b.at[c],
                send_sem=s3_send.at[1, c], recv_sem=s3_recv.at[1, c], device_id={'dp': xnbr}),
        )

    def stage2(c, pp_ref):
        s1_copy(c, pp_ref).wait_recv()
        for q in range(4):
            r1[c, q // 2, q % 2] += pp_ref[core, q // 2, q % 2]
        for cp in s2_copies(c):
            cp.start()

    def stage3(c):
        first, second = s2_copies(c)
        first.wait_recv()
        for q in range(2):
            r2a[c, q] += r1[c, q, xx, :, 0:HALF]
        second.wait_recv()
        for q in range(2):
            r2b[c, q] += r1[c, yy, q, :, HALF:CW]
        for cp in s3_copies(c):
            cp.start()

    def stage4(c):
        first, second = s3_copies(c)
        base = pl.multiple_of(c * CW, CW)
        first.wait_recv()
        de_ref[:, pl.ds(base, HALF)] = r2a[c, yy] + r3a[c]
        second.wait_recv()
        de_ref[:, pl.ds(pl.multiple_of(base + HALF, HALF), HALF)] = r2b[c, xx] + r3b[c]

    nsub = TOK // RG

    def wait_in(i):
        for cp in fetch(i):
            cp.wait()

    def both(i, dr_new, dr_old, pp_ref, cuts=6):
        for k in range(cuts):
            if k < 2:
                emb_piece(dr_old, pp_ref, k)
            else:
                hid_piece(i - 1, dr_old, k - 2)
            elementwise(i, dr_new, nsub * k // cuts, nsub * (k + 1) // cuts)

    wait_in(0)
    start_fetch(2)
    elementwise(0, dr0, 0, nsub)
    wait_in(1)
    start_fetch(3)
    both(1, dr1, dr0, pp0)
    s1_copy(0, pp0).start()

    def pair(t, carry):
        for par, (dr_new, dr_old, pp_new, pp_old) in enumerate(((dr0, dr1, pp1, pp0), (dr1, dr0, pp0, pp1))):
            i = 2 + 2 * t + par
            wait_in(i)

            @pl.when(i + 2 < NCH)
            def _():
                start_fetch(i + 2)

            @pl.when(i >= 3)
            def _():
                s1_copy(i - 3, pp_new).wait_send()

            both(i, dr_new, dr_old, pp_new)
            s1_copy(i - 1, pp_new).start()
            stage2(i - 2, pp_old)
        return carry

    lax.fori_loop(0, (NCH - 2) // 2, pair, 0)
    s1_copy(NCH - 3, pp1).wait_send()
    for k in range(2):
        emb_piece(dr1, pp1, k)
    s1_copy(NCH - 1, pp1).start()
    for k in range(4):
        hid_piece(NCH - 1, dr1, k)

    def where_of(h):
        pos = z if h == 0 else 3 - z
        up = z + 1 if h == 0 else z - 1
        down = z - 1 if h == 0 else z + 1
        return pos, up, down

    def lanes(h, b):
        lo = h * 512 + b * 128
        return slice(lo, lo + 128)

    def ar_first(h, b):
        pos, up, _ = where_of(h)
        idx = 4 * h + b
        return pltpu.make_async_remote_copy(
            src_ref=dg_ref.at[:, pl.ds(h * 512 + b * 128, 128)], dst_ref=ar_in.at[idx],
            send_sem=ar_send.at[idx], recv_sem=ar_recv.at[idx], device_id={'tp': up})

    def ar_next(h, b):
        pos, up, _ = where_of(h)
        idx = 4 * h + b
        return pltpu.make_async_remote_copy(
            src_ref=ar_in.at[idx], dst_ref=ar_in.at[idx],
            send_sem=ar_send.at[idx], recv_sem=ar_recv.at[idx], device_id={'tp': up})

    def bc_copy(h, b):
        _, _, down = where_of(h)
        idx = 4 * h + b
        part = dh_f.at[:, pl.ds(h * 512 + b * 128, 128)]
        return pltpu.make_async_remote_copy(
            src_ref=part, dst_ref=part,
            send_sem=bc_send.at[idx], recv_sem=bc_recv.at[idx], device_id={'tp': down})

    for b in range(4):
        for h in range(2):
            @pl.when(where_of(h)[0] == 0)
            def _():
                ar_first(h, b).start()

    def reduce_step(h, b):
        pos, _, _ = where_of(h)
        idx = 4 * h + b

        @pl.when(pos > 0)
        def _():
            ar_next(h, b).wait_recv()

            @pl.when(pos < 3)
            def _():
                ar_in[idx] += dg_ref[:, lanes(h, b)]
                ar_next(h, b).start()

            @pl.when(pos == 3)
            def _():
                dg = ar_in[idx] + dg_ref[:, lanes(h, b)]
                x = hid_ref[:, lanes(h, b)].astype(F32)
                inv = lax.rsqrt(jnp.mean(x * x, axis=0, keepdims=True) + NORM_EPS)
                dw_ref[...] += dg * (x * inv)
                du = dg * (1.0 + w_ref[...])
                inner = jnp.sum(du * x, axis=0, keepdims=True)
                dh_f[:, lanes(h, b)] = du * inv - x * (inv * inv * inv * inner * (1.0 / D))
                bc_copy(h, b).start()

    def spread_step(h, b):
        pos, _, _ = where_of(h)

        @pl.when(pos < 3)
        def _():
            bc_copy(h, b).wait_recv()

            @pl.when(pos > 0)
            def _():
                bc_copy(h, b).start()

        dh_ref[:, lanes(h, b)] = dh_f[:, lanes(h, b)].astype(BF16)

    stage2(NCH - 2, pp0)
    stage2(NCH - 1, pp1)

    def loop(lo, hi, fn):
        def body(c, carry):
            fn(c)
            return carry
        lax.fori_loop(lo, hi, body, 0)

    loop(0, 8, stage3)
    for b in range(4):
        reduce_step(0, b)
        reduce_step(1, b)
        loop(8 + 4 * b, 12 + 4 * b, stage3)
    for b in range(4):
        spread_step(0, b)
        spread_step(1, b)
        loop(6 * b, 6 * b + 6, stage4)

    def wsum(k, carry):
        rows = pl.ds(pl.multiple_of(k * 8, 8), 8)
        return carry + wgt[rows, :] * kl_acc[rows, :]

    kl_tile = lax.fori_loop(0, TOK // 8, wsum, jnp.zeros((8, 128), F32))
    loss_ref[...] = kl_tile + lse_sum * (1.0 / 1024.0)

    for k in range(1, 4):
        st_copy(k).wait_send()
    for k in range(1, 8):
        cnt_copy(k).wait_send()
    s1_copy(NCH - 2, pp0).wait_send()
    s1_copy(NCH - 1, pp1).wait_send()

    def drain(c):
        for cp in s2_copies(c) + s3_copies(c):
            cp.wait_send()

    loop(0, NCH, drain)
    for h in range(2):
        pos = where_of(h)[0]
        for b in range(4):
            @pl.when(pos < 3)
            def _():
                ar_next(h, b).wait_send()

            @pl.when(pos > 0)
            def _():
                bc_copy(h, b).wait_send()


def second_pass(th, teach, emb_t, g_t, hid_t, w_col, stats, mask_row):
    vmem = pl.BlockSpec(memory_space=pltpu.VMEM)
    hbm = pl.BlockSpec(memory_space=pl.ANY)
    dma = pltpu.SemaphoreType.DMA
    return pl.pallas_call(
        grad_kernel,
        out_shape=(
            jax.ShapeDtypeStruct((GRP, VLOC), F32),
            jax.ShapeDtypeStruct((D, TOK), BF16),
            jax.ShapeDtypeStruct((D, 128), F32),
            jax.ShapeDtypeStruct((8, 128), F32),
        ),
        in_specs=[hbm] * 3 + [vmem] * 5,
        out_specs=(vmem,) * 4,
        scratch_shapes=[
            pltpu.VMEM((3, TOK, CW), F32),
            pltpu.VMEM((3, TOK, CW), BF16),
            pltpu.VMEM((4, D, CW), BF16),
            pltpu.VMEM((TOK, CW), BF16),
            pltpu.VMEM((TOK, CW), BF16),
            pltpu.VMEM((2, 2, 2, GRP, CW), F32),
            pltpu.VMEM((2, 2, 2, GRP, CW), F32),
            pltpu.VMEM((NCH, 2, 2, GRP, CW), F32),
            pltpu.VMEM((NCH, 2, GRP, HALF), F32),
            pltpu.VMEM((NCH, 2, GRP, HALF), F32),
            pltpu.VMEM((NCH, GRP, HALF), F32),
            pltpu.VMEM((NCH, GRP, HALF), F32),
            pltpu.VMEM((D, TOK), F32),
            pltpu.VMEM((8, D, 128), F32),
            pltpu.VMEM((D, TOK), F32),
            pltpu.VMEM((4, 8, TOK), F32),
            pltpu.VMEM((8, 8, 128), F32),
            pltpu.VMEM((8, 128), F32),
        ] + [pltpu.VMEM((TOK, 128), F32)] * 5 + [
            dma((3, 4)), dma((4,)), dma((4,)), dma((8,)), dma((8,)),
            dma((NCH,)), dma((NCH,)), dma((2, NCH)), dma((2, NCH)), dma((2, NCH)), dma((2, NCH)),
            dma((8,)), dma((8,)), dma((8,)), dma((8,)),
        ],
        compiler_params=pltpu.CompilerParams(
            collective_id=0, has_side_effects=True, vmem_limit_bytes=67_000_000),
        cost_estimate=pl.CostEstimate(
            flops=4 * TOK * VLOC * D, bytes_accessed=100_000_000, transcendentals=2 * TOK * VLOC),
    )(th, teach, emb_t, g_t, hid_t, w_col, stats, mask_row)


def solution(mesh):
    def device_fn(hid_loc, norm_w, emb_loc, teach_loc, mask_loc):
        hid_t = hid_loc.T
        emb_t = emb_loc.T
        w_col = norm_w.astype(F32).reshape(D, 1)
        mask_row = mask_loc.astype(F32).reshape(1, TOK)
        th, g_t, stats = first_pass(hid_t, w_col, emb_t, teach_loc)
        de_t, dh_t, dw_part, loss_part = second_pass(th, teach_loc, emb_t, g_t, hid_t, w_col, stats, mask_row)
        packed = jnp.concatenate([jnp.sum(dw_part, axis=1), jnp.sum(loss_part).reshape(1)])
        total = lax.psum(packed, ('tp', 'dp'))
        return total[D], dh_t.T, de_t.T, total[:D]

    return jax.shard_map(device_fn, mesh=mesh, in_specs=(P('dp', None), P(None), P('tp', None), P('dp', 'tp'), P('dp')), out_specs=(P(), P('dp', None), P('tp', 'dp'), P(None)), check_vma=False)
```

```python
import jax
import jax.numpy as jnp
from jax import lax
from jax.experimental import pallas as pl
from jax.experimental.pallas import tpu as pltpu
from jax.sharding import PartitionSpec as P

SOFT_CAP = 30.0
NORM_EPS = 1e-6
LOG2E = 1.4426950408889634
LN2 = 0.6931471805599453
CAP2 = SOFT_CAP * LOG2E
D = 576
GRP = 72
TOK = 1024
VLOC = 12288
CW = 512
HALF = CW // 2
NCH = VLOC // CW
CWA = 512
NCHA = VLOC // CWA
RG = 32
F32 = jnp.float32
BF16 = jnp.bfloat16
NT = (((1,), (1,)), ((), ()))


def lane_tiles(arr):
    return [arr[:, k * 128:(k + 1) * 128] for k in range(arr.shape[1] // 128)]


def tree(op, parts):
    while len(parts) > 1:
        parts = [op(parts[k], parts[k + 1]) if k + 1 < len(parts) else parts[k] for k in range(0, len(parts), 2)]
    return parts[0]


def stats_kernel(hid_ref, w_ref, emb_ref, tea_ref, th_ref, gt_ref, st_ref, g_scr, s_acc, m_acc, t_acc):
    step = pl.program_id(0)

    @pl.when(step == 0)
    def _():
        x = hid_ref[...].astype(F32)
        inv = lax.rsqrt(jnp.mean(x * x, axis=0, keepdims=True) + NORM_EPS)
        gn = x * inv * (1.0 + w_ref[...])
        gt_ref[...] = gn.astype(BF16)
        g_scr[...] = jnp.transpose(gn).astype(BF16)
        s_acc[...] = jnp.zeros_like(s_acc)
        t_acc[...] = jnp.zeros_like(t_acc)
        m_acc[...] = jnp.full_like(m_acc, -jnp.inf)

    tb = 256
    for blk in range(TOK // tb):
        raw = jnp.dot(g_scr[blk * tb:(blk + 1) * tb, :], emb_ref[...], preferred_element_type=F32)
        for sub in range(tb // RG):
            rows = slice(blk * tb + sub * RG, blk * tb + (sub + 1) * RG)
            th = jnp.tanh(raw[sub * RG:(sub + 1) * RG, :] * (1.0 / SOFT_CAP))
            th_ref[rows, :] = th
            s_acc[rows, :] += tree(jnp.add, lane_tiles(jnp.exp2(th * CAP2 - CAP2)))
            tea = lane_tiles(tea_ref[rows, :].astype(F32))
            old = m_acc[rows, :]
            new = jnp.maximum(old, tree(jnp.maximum, tea))
            m_acc[rows, :] = new
            t_acc[rows, :] = t_acc[rows, :] * jnp.exp2((old - new) * LOG2E) + tree(
                jnp.add, [jnp.exp2((part - new) * LOG2E) for part in tea])

    @pl.when(step == NCHA - 1)
    def _():
        s_row = jnp.sum(jnp.transpose(s_acc[...]), axis=0, keepdims=True)
        m_t = jnp.transpose(m_acc[...])
        m_row = jnp.max(m_t, axis=0, keepdims=True)
        t_row = jnp.sum(jnp.transpose(t_acc[...]) * jnp.exp2((m_t - m_row) * LOG2E), axis=0, keepdims=True)
        st_ref[...] = jnp.concatenate([s_row, m_row, t_row, jnp.zeros((5, TOK), F32)], axis=0)


def first_pass(hid_t, w_col, emb_t, teach):
    return pl.pallas_call(
        stats_kernel,
        grid=(NCHA,),
        out_shape=(
            jax.ShapeDtypeStruct((TOK, VLOC), F32),
            jax.ShapeDtypeStruct((D, TOK), BF16),
            jax.ShapeDtypeStruct((8, TOK), F32),
        ),
        in_specs=[
            pl.BlockSpec((D, TOK), lambda i: (0, 0)),
            pl.BlockSpec((D, 1), lambda i: (0, 0)),
            pl.BlockSpec((D, CWA), lambda i: (0, i)),
            pl.BlockSpec((TOK, CWA), lambda i: (0, i)),
        ],
        out_specs=(
            pl.BlockSpec((TOK, CWA), lambda i: (0, i)),
            pl.BlockSpec((D, TOK), lambda i: (0, 0)),
            pl.BlockSpec((8, TOK), lambda i: (0, 0)),
        ),
        scratch_shapes=[pltpu.VMEM((TOK, D), BF16)] + [pltpu.VMEM((TOK, 128), F32)] * 3,
        compiler_params=pltpu.CompilerParams(
            dimension_semantics=("arbitrary",), vmem_limit_bytes=48 * 1024 * 1024),
        cost_estimate=pl.CostEstimate(
            flops=2 * TOK * VLOC * D, bytes_accessed=90_000_000, transcendentals=3 * TOK * VLOC),
    )(hid_t, w_col, emb_t, teach)


def grad_kernel(th_hbm, tea_hbm, emb_hbm, gt_ref, hid_ref, w_ref, st_ref, mask_ref,
                de_ref, dh_ref, small_ref,
                th_buf, tea_buf, emb_buf, dr0, dr1, pp0, pp1, r1, r2a, r2b, r3a, r3b,
                dg_ref, ar_in, dh_f, st_in, cnt_in, cnt_own, dw_acc, sm_dp, sm_tp, wgt, l2s, mtx, l2t, kl_acc,
                in_sem, st_send, st_recv, cnt_send, cnt_recv,
                s1_send, s1_recv, s2_send, s2_recv, s3_send, s3_recv,
                ar_send, ar_recv, bc_send, bc_recv, smd_send, smd_recv, smt_send, smt_recv):
    z = lax.axis_index('tp')
    d = lax.axis_index('dp')
    core = d % 2
    xx = (d // 2) % 2
    yy = d // 4
    partner = d + 1 - 2 * core
    xnbr = d + 2 - 4 * xx
    ynbr = d + 4 - 8 * yy

    def fetch(i):
        cols = pl.ds(pl.multiple_of(i * CW, CW), CW)
        three = i % 3
        four = i % 4
        return (
            pltpu.make_async_copy(th_hbm.at[:, cols], th_buf.at[three], in_sem.at[0, three]),
            pltpu.make_async_copy(tea_hbm.at[:, cols], tea_buf.at[three], in_sem.at[1, three]),
            pltpu.make_async_copy(emb_hbm.at[:, cols], emb_buf.at[four], in_sem.at[2, four]),
        )

    def start_fetch(i):
        for cp in fetch(i):
            cp.start()

    start_fetch(0)
    start_fetch(1)

    barrier = pltpu.get_barrier_semaphore()
    for k in range(1, 4):
        pl.semaphore_signal(barrier, inc=1, device_id={'tp': (z + k) % 4})
    for k in range(1, 8):
        pl.semaphore_signal(barrier, inc=1, device_id={'dp': (d + k) % 8})
    cnt_own[...] = jnp.full((8, 128), jnp.sum(mask_ref[...]), F32)
    pl.semaphore_wait(barrier, 10)

    def st_copy(k):
        return pltpu.make_async_remote_copy(
            src_ref=st_ref, dst_ref=st_in.at[k], send_sem=st_send.at[k], recv_sem=st_recv.at[k],
            device_id={'tp': (z + k) % 4})

    def cnt_copy(k):
        return pltpu.make_async_remote_copy(
            src_ref=cnt_own, dst_ref=cnt_in.at[k], send_sem=cnt_send.at[k], recv_sem=cnt_recv.at[k],
            device_id={'dp': (d + k) % 8})

    for k in range(1, 4):
        st_copy(k).start()
    for k in range(1, 8):
        cnt_copy(k).start()
    dg_ref[...] = jnp.zeros_like(dg_ref)
    kl_acc[...] = jnp.zeros_like(kl_acc)
    dw_acc[...] = jnp.zeros_like(dw_acc)
    for k in range(1, 4):
        st_copy(k).wait_recv()
    for k in range(1, 8):
        cnt_copy(k).wait_recv()

    stats = [st_ref[...]] + [st_in[k] for k in range(1, 4)]
    s_tot = tree(jnp.add, [st[0:1, :] for st in stats])
    m_tot = tree(jnp.maximum, [st[1:2, :] for st in stats])
    t_tot = tree(jnp.add, [st[2:3, :] * jnp.exp2((st[1:2, :] - m_tot) * LOG2E) for st in stats])
    count = cnt_own[0:1, :]
    for k in range(1, 8):
        count = count + cnt_in[k][0:1, :]
    w_row = mask_ref[...] / jnp.concatenate([count] * (TOK // 128), axis=1)
    l2s_row = jnp.log2(s_tot) + CAP2
    l2t_row = jnp.log2(t_tot)

    def to_rows(row):
        return jnp.transpose(jnp.broadcast_to(row, (128, TOK)))

    wgt[...] = to_rows(w_row)
    l2s[...] = to_rows(l2s_row)
    mtx[...] = to_rows(m_tot)
    l2t[...] = to_rows(l2t_row)
    lse_part = w_row * ((l2s_row - l2t_row) * LN2 - m_tot)
    lse_sum = jnp.where(z == 0, jnp.sum(lse_part), 0.0)

    def elementwise(i, dr_ref, lo, hi):
        slot = i % 3
        for sub in range(lo, hi):
            rows = slice(sub * RG, (sub + 1) * RG)
            w_b, ls_b, m_b, lt_b = wgt[rows, :], l2s[rows, :], mtx[rows, :], l2t[rows, :]
            kl = []
            for q in range(CW // 128):
                cols = slice(q * 128, (q + 1) * 128)
                th = th_buf[slot, rows, cols]
                tea = tea_buf[slot, rows, cols].astype(F32)
                p_s = jnp.exp2(th * CAP2 - ls_b)
                p_t = jnp.exp2((tea - m_b) * LOG2E - lt_b)
                kl.append(p_t * (tea - SOFT_CAP * th))
                dr_ref[rows, cols] = ((p_s - p_t) * w_b * (1.0 - th * th)).astype(BF16)
            kl_acc[rows, :] += tree(jnp.add, kl)

    def emb_piece(dr_ref, pp_ref, k):
        part = jnp.dot(gt_ref[...], dr_ref[:, k * HALF:(k + 1) * HALF], preferred_element_type=F32)
        for grp in range(8):
            pp_ref[grp % 2, grp // 4, (grp // 2) % 2, :, k * HALF:(k + 1) * HALF] = part[grp * GRP:(grp + 1) * GRP, :]

    def hid_piece(i, dr_ref, k):
        cols = slice(k * 256, (k + 1) * 256)
        dg_ref[:, cols] += lax.dot_general(emb_buf[i % 4], dr_ref[cols, :], NT, preferred_element_type=F32)

    def s1_copy(c, pp_ref):
        return pltpu.make_async_remote_copy(
            src_ref=pp_ref.at[1 - core], dst_ref=r1.at[c], send_sem=s1_send.at[c], recv_sem=s1_recv.at[c],
            device_id={'dp': partner})

    def s2_copies(c):
        return (
            pltpu.make_async_remote_copy(
                src_ref=r1.at[c, :, 1 - xx, :, pl.ds(0, HALF)], dst_ref=r2a.at[c],
                send_sem=s2_send.at[0, c], recv_sem=s2_recv.at[0, c], device_id={'dp': xnbr}),
            pltpu.make_async_remote_copy(
                src_ref=r1.at[c, 1 - yy, :, :, pl.ds(HALF, HALF)], dst_ref=r2b.at[c],
                send_sem=s2_send.at[1, c], recv_sem=s2_recv.at[1, c], device_id={'dp': ynbr}),
        )

    def s3_copies(c):
        return (
            pltpu.make_async_remote_copy(
                src_ref=r2a.at[c, 1 - yy], dst_ref=r3a.at[c],
                send_sem=s3_send.at[0, c], recv_sem=s3_recv.at[0, c], device_id={'dp': ynbr}),
            pltpu.make_async_remote_copy(
                src_ref=r2b.at[c, 1 - xx], dst_ref=r3b.at[c],
                send_sem=s3_send.at[1, c], recv_sem=s3_recv.at[1, c], device_id={'dp': xnbr}),
        )

    def stage1(c, pp_ref):
        s1_copy(c, pp_ref).wait_recv()
        for q in range(4):
            r1[c, q // 2, q % 2] += pp_ref[core, q // 2, q % 2]

    def stage2(c):
        for cp in s2_copies(c):
            cp.start()

    def stage3(c):
        first, second = s2_copies(c)
        first.wait_recv()
        for q in range(2):
            r2a[c, q] += r1[c, q, xx, :, 0:HALF]
        second.wait_recv()
        for q in range(2):
            r2b[c, q] += r1[c, yy, q, :, HALF:CW]
        for cp in s3_copies(c):
            cp.start()

    def stage4(c):
        first, second = s3_copies(c)
        base = pl.multiple_of(c * CW, CW)
        first.wait_recv()
        de_ref[:, pl.ds(base, HALF)] = r2a[c, yy] + r3a[c]
        second.wait_recv()
        de_ref[:, pl.ds(pl.multiple_of(base + HALF, HALF), HALF)] = r2b[c, xx] + r3b[c]

    nsub = TOK // RG

    def wait_in(i):
        for cp in fetch(i):
            cp.wait()

    def both(i, dr_new, dr_old, pp_ref, cuts=6):
        for k in range(cuts):
            if k < 2:
                emb_piece(dr_old, pp_ref, k)
            else:
                hid_piece(i - 1, dr_old, k - 2)
            elementwise(i, dr_new, nsub * k // cuts, nsub * (k + 1) // cuts)

    wait_in(0)
    start_fetch(2)
    elementwise(0, dr0, 0, nsub)
    wait_in(1)
    start_fetch(3)
    both(1, dr1, dr0, pp0)
    s1_copy(0, pp0).start()

    def tick(t):
        stage2(t + 1)
        stage3(t - 1)

        @pl.when(t >= 3)
        def _():
            stage4(t - 3)

    def pair(t, carry):
        for par, (dr_new, dr_old, pp_new, pp_old) in enumerate(((dr0, dr1, pp1, pp0), (dr1, dr0, pp0, pp1))):
            i = 2 + 2 * t + par
            wait_in(i)

            @pl.when(i + 2 < NCH)
            def _():
                start_fetch(i + 2)

            @pl.when(i >= 3)
            def _():
                s1_copy(i - 3, pp_new).wait_send()

            both(i, dr_new, dr_old, pp_new)
            s1_copy(i - 1, pp_new).start()
            stage1(i - 2, pp_old)
            if par == 0:
                @pl.when(t == 0)
                def _():
                    stage2(0)

                @pl.when(t > 0)
                def _():
                    tick(t)
            else:
                @pl.when(t == 0)
                def _():
                    stage2(1)
        return carry

    npair = (NCH - 2) // 2
    lax.fori_loop(0, npair, pair, 0)
    s1_copy(NCH - 3, pp1).wait_send()
    for k in range(2):
        emb_piece(dr1, pp1, k)
    s1_copy(NCH - 1, pp1).start()
    for k in range(4):
        hid_piece(NCH - 1, dr1, k)

    def where_of(h):
        pos = z if h == 0 else 3 - z
        up = z + 1 if h == 0 else z - 1
        down = z - 1 if h == 0 else z + 1
        return pos, up, down

    def lanes(h, b):
        lo = h * 512 + b * 128
        return slice(lo, lo + 128)

    def ar_first(h, b):
        pos, up, _ = where_of(h)
        idx = 4 * h + b
        return pltpu.make_async_remote_copy(
            src_ref=dg_ref.at[:, pl.ds(h * 512 + b * 128, 128)], dst_ref=ar_in.at[idx],
            send_sem=ar_send.at[idx], recv_sem=ar_recv.at[idx], device_id={'tp': up})

    def ar_next(h, b):
        pos, up, _ = where_of(h)
        idx = 4 * h + b
        return pltpu.make_async_remote_copy(
            src_ref=ar_in.at[idx], dst_ref=ar_in.at[idx],
            send_sem=ar_send.at[idx], recv_sem=ar_recv.at[idx], device_id={'tp': up})

    def bc_copy(h, b):
        _, _, down = where_of(h)
        idx = 4 * h + b
        part = dh_f.at[:, pl.ds(h * 512 + b * 128, 128)]
        return pltpu.make_async_remote_copy(
            src_ref=part, dst_ref=part,
            send_sem=bc_send.at[idx], recv_sem=bc_recv.at[idx], device_id={'tp': down})

    for b in range(4):
        for h in range(2):
            @pl.when(where_of(h)[0] == 0)
            def _():
                ar_first(h, b).start()

    def add_on(h, b):
        idx = 4 * h + b
        ar_next(h, b).wait_recv()
        ar_in[idx] += dg_ref[:, lanes(h, b)]
        ar_next(h, b).start()

    def finish(h, b):
        ar_next(h, b).wait_recv()
        dg = ar_in[4 * h + b] + dg_ref[:, lanes(h, b)]
        x = hid_ref[:, lanes(h, b)].astype(F32)
        inv = lax.rsqrt(jnp.mean(x * x, axis=0, keepdims=True) + NORM_EPS)
        dw_acc[...] += dg * (x * inv)
        du = dg * (1.0 + w_ref[...])
        inner = jnp.sum(du * x, axis=0, keepdims=True)
        dh_f[:, lanes(h, b)] = du * inv - x * (inv * inv * inv * inner * (1.0 / D))
        bc_copy(h, b).start()

    def spread(h, b, pos):
        bc_copy(h, b).wait_recv()
        if pos > 0:
            bc_copy(h, b).start()

    def slot(s):
        for pos in (1, 2, 3):
            b = s - (pos - 1)
            if 0 <= b < 4:
                for h in range(2):
                    @pl.when(where_of(h)[0] == pos)
                    def _():
                        if pos < 3:
                            add_on(h, b)
                        else:
                            finish(h, b)
        for pos in (2, 1, 0):
            b = s - 4 - (2 - pos)
            if 0 <= b < 4:
                for h in range(2):
                    @pl.when(where_of(h)[0] == pos)
                    def _():
                        spread(h, b, pos)

    def wsum(k, carry):
        rows = pl.ds(pl.multiple_of(k * 8, 8), 8)
        return carry + wgt[rows, :] * kl_acc[rows, :]

    def small_copy(k, over):
        mine, size, buf, send, recv = (
            (d, 8, sm_dp, smd_send, smd_recv) if over == 'dp' else (z, 4, sm_tp, smt_send, smt_recv))
        peer = (mine + k) % size
        return pltpu.make_async_remote_copy(
            src_ref=buf.at[mine], dst_ref=buf.at[mine], send_sem=send.at[k], recv_sem=recv.at[mine],
            device_id={over: peer})

    def small_wait(k, over):
        mine, size, buf, send, recv = (
            (d, 8, sm_dp, smd_send, smd_recv) if over == 'dp' else (z, 4, sm_tp, smt_send, smt_recv))
        peer = (mine + k) % size
        pltpu.make_async_remote_copy(
            src_ref=buf.at[peer], dst_ref=buf.at[peer], send_sem=send.at[k], recv_sem=recv.at[peer],
            device_id={over: peer}).wait_recv()

    def small_dp():
        kl_tile = lax.fori_loop(0, TOK // 8, wsum, jnp.zeros((8, 128), F32))
        loss = jnp.sum(kl_tile) + lse_sum
        dw_row = jnp.sum(jnp.transpose(dw_acc[...]), axis=0, keepdims=True)
        sm_dp[d] = jnp.concatenate([dw_row, jnp.full((1, D), loss, F32), jnp.zeros((6, D), F32)], axis=0)
        for k in range(1, 8):
            small_copy(k, 'dp').start()

    def small_tp():
        for k in range(1, 8):
            small_wait(k, 'dp')
        sm_tp[z] = tree(jnp.add, [sm_dp[k] for k in range(8)])
        for k in range(1, 4):
            small_copy(k, 'tp').start()

    def small_end():
        for k in range(1, 4):
            small_wait(k, 'tp')
        small_ref[...] = tree(jnp.add, [sm_tp[k] for k in range(4)])

    def ticks(lo, hi):
        def body(t, carry):
            tick(t)
            return carry
        lax.fori_loop(lo, hi, body, 0)

    stage1(NCH - 2, pp0)
    stage1(NCH - 1, pp1)
    t0 = npair
    ticks(t0, t0 + 2)
    slot(0)
    ticks(t0 + 2, t0 + 3)
    slot(1)
    ticks(t0 + 3, t0 + 4)
    slot(2)
    ticks(t0 + 4, t0 + 6)
    slot(3)
    ticks(t0 + 6, t0 + 7)
    slot(4)
    ticks(t0 + 7, t0 + 8)
    slot(5)
    ticks(t0 + 8, t0 + 10)
    slot(6)
    small_dp()
    ticks(t0 + 10, t0 + 11)
    slot(7)
    ticks(t0 + 11, NCH - 1)
    slot(8)
    small_tp()
    stage3(NCH - 2)
    stage4(NCH - 4)
    stage3(NCH - 1)
    stage4(NCH - 3)
    slot(9)
    dh_ref[...] = dh_f[...].astype(BF16)
    stage4(NCH - 2)
    stage4(NCH - 1)
    small_end()

    for k in range(1, 4):
        st_copy(k).wait_send()
    for k in range(1, 8):
        cnt_copy(k).wait_send()
    s1_copy(NCH - 2, pp0).wait_send()
    s1_copy(NCH - 1, pp1).wait_send()

    def drain(c):
        for cp in s2_copies(c) + s3_copies(c):
            cp.wait_send()

    def drain_body(c, carry):
        drain(c)
        return carry

    lax.fori_loop(0, NCH, drain_body, 0)
    for k in range(1, 8):
        small_copy(k, 'dp').wait_send()
    for k in range(1, 4):
        small_copy(k, 'tp').wait_send()
    for h in range(2):
        pos = where_of(h)[0]
        for b in range(4):
            @pl.when(pos < 3)
            def _():
                ar_next(h, b).wait_send()

            @pl.when(pos > 0)
            def _():
                bc_copy(h, b).wait_send()


def second_pass(th, teach, emb_t, g_t, hid_t, w_col, stats, mask_row):
    vmem = pl.BlockSpec(memory_space=pltpu.VMEM)
    hbm = pl.BlockSpec(memory_space=pl.ANY)
    dma = pltpu.SemaphoreType.DMA
    return pl.pallas_call(
        grad_kernel,
        out_shape=(
            jax.ShapeDtypeStruct((GRP, VLOC), F32),
            jax.ShapeDtypeStruct((D, TOK), BF16),
            jax.ShapeDtypeStruct((8, D), F32),
        ),
        in_specs=[hbm] * 3 + [vmem] * 5,
        out_specs=(vmem,) * 3,
        scratch_shapes=[
            pltpu.VMEM((3, TOK, CW), F32),
            pltpu.VMEM((3, TOK, CW), BF16),
            pltpu.VMEM((4, D, CW), BF16),
            pltpu.VMEM((TOK, CW), BF16),
            pltpu.VMEM((TOK, CW), BF16),
            pltpu.VMEM((2, 2, 2, GRP, CW), F32),
            pltpu.VMEM((2, 2, 2, GRP, CW), F32),
            pltpu.VMEM((NCH, 2, 2, GRP, CW), F32),
            pltpu.VMEM((NCH, 2, GRP, HALF), F32),
            pltpu.VMEM((NCH, 2, GRP, HALF), F32),
            pltpu.VMEM((NCH, GRP, HALF), F32),
            pltpu.VMEM((NCH, GRP, HALF), F32),
            pltpu.VMEM((D, TOK), F32),
            pltpu.VMEM((8, D, 128), F32),
            pltpu.VMEM((D, TOK), F32),
            pltpu.VMEM((4, 8, TOK), F32),
            pltpu.VMEM((8, 8, 128), F32),
            pltpu.VMEM((8, 128), F32),
            pltpu.VMEM((D, 128), F32),
            pltpu.VMEM((8, 8, D), F32),
            pltpu.VMEM((4, 8, D), F32),
        ] + [pltpu.VMEM((TOK, 128), F32)] * 5 + [
            dma((3, 4)), dma((4,)), dma((4,)), dma((8,)), dma((8,)),
            dma((NCH,)), dma((NCH,)), dma((2, NCH)), dma((2, NCH)), dma((2, NCH)), dma((2, NCH)),
            dma((8,)), dma((8,)), dma((8,)), dma((8,)),
            dma((8,)), dma((8,)), dma((4,)), dma((4,)),
        ],
        compiler_params=pltpu.CompilerParams(
            collective_id=0, has_side_effects=True, vmem_limit_bytes=67_000_000),
        cost_estimate=pl.CostEstimate(
            flops=4 * TOK * VLOC * D, bytes_accessed=100_000_000, transcendentals=2 * TOK * VLOC),
    )(th, teach, emb_t, g_t, hid_t, w_col, stats, mask_row)


def solution(mesh):
    def device_fn(hid_loc, norm_w, emb_loc, teach_loc, mask_loc):
        hid_t = hid_loc.T
        emb_t = emb_loc.T
        w_col = norm_w.astype(F32).reshape(D, 1)
        mask_row = mask_loc.astype(F32).reshape(1, TOK)
        th, g_t, stats = first_pass(hid_t, w_col, emb_t, teach_loc)
        de_t, dh_t, small = second_pass(th, teach_loc, emb_t, g_t, hid_t, w_col, stats, mask_row)
        return small[1, 0], dh_t.T, de_t.T, small[0]

    return jax.shard_map(device_fn, mesh=mesh, in_specs=(P('dp', None), P(None), P('tp', None), P('dp', 'tp'), P('dp')), out_specs=(P(), P('dp', None), P('tp', 'dp'), P(None)), check_vma=False)
```

```python
import jax
import jax.numpy as jnp
from jax import lax
from jax.experimental import pallas as pl
from jax.experimental.pallas import tpu as pltpu
from jax.sharding import PartitionSpec as P

SOFT_CAP = 30.0
NORM_EPS = 1e-6
LOG2E = 1.4426950408889634
LN2 = 0.6931471805599453
CAP2 = SOFT_CAP * LOG2E
D = 576
GRP = 72
TOK = 1024
VLOC = 12288
CW = 512
HALF = CW // 2
NCH = VLOC // CW
RG = 32
TB1 = 128
TB2 = 512
F32 = jnp.float32
BF16 = jnp.bfloat16
NT = (((1,), (1,)), ((), ()))


def lane_tiles(arr):
    return [arr[:, k * 128:(k + 1) * 128] for k in range(arr.shape[1] // 128)]


def tree(op, parts):
    while len(parts) > 1:
        parts = [op(parts[k], parts[k + 1]) if k + 1 < len(parts) else parts[k] for k in range(0, len(parts), 2)]
    return parts[0]


def grad_kernel(tea_hbm, emb_hbm, hid_ref, w_ref, mask_ref,
                th_hbm, de_ref, dh_ref, small_ref,
                g_scr, gt_ref, st_ref, out_sem,
                th_buf, tea_buf, emb_buf, dr, pp0, pp1, r1, r2a, r2b, r3a, r3b,
                dg_ref, ar_in, dh_f, st_in, cnt_in, cnt_own, dw_acc, sm_dp, sm_tp, wgt, l2s, mtx, l2t, kl_acc,
                in_sem, st_send, st_recv, cnt_send, cnt_recv,
                s1_send, s1_recv, s2_send, s2_recv, s3_send, s3_recv,
                ar_send, ar_recv, bc_send, bc_recv, smd_send, smd_recv, smt_send, smt_recv):
    z = lax.axis_index('tp')
    d = lax.axis_index('dp')
    core = d % 2
    xx = (d // 2) % 2
    yy = d // 4
    partner = d + 1 - 2 * core
    xnbr = d + 2 - 4 * xx
    ynbr = d + 4 - 8 * yy

    def fetch(i):
        cols = pl.ds(pl.multiple_of(i * CW, CW), CW)
        three = i % 3
        return (
            pltpu.make_async_copy(th_hbm.at[:, cols], th_buf.at[three], in_sem.at[0, three]),
            pltpu.make_async_copy(tea_hbm.at[:, cols], tea_buf.at[three], in_sem.at[1, three]),
            pltpu.make_async_copy(emb_hbm.at[:, cols], emb_buf.at[three], in_sem.at[2, three]),
        )

    def start_fetch(i):
        for cp in fetch(i):
            cp.start()

    def fetch_tea(i):
        cols = pl.ds(pl.multiple_of(i * CW, CW), CW)
        three = i % 3
        return (
            pltpu.make_async_copy(tea_hbm.at[:, cols], tea_buf.at[three], in_sem.at[1, three]),
            pltpu.make_async_copy(emb_hbm.at[:, cols], emb_buf.at[three], in_sem.at[2, three]),
        )

    def put_th(i):
        cols = pl.ds(pl.multiple_of(i * CW, CW), CW)
        three = i % 3
        return pltpu.make_async_copy(th_buf.at[three], th_hbm.at[:, cols], out_sem.at[three])

    for k in range(2):
        for cp in fetch_tea(k):
            cp.start()

    barrier = pltpu.get_barrier_semaphore()
    for k in range(1, 4):
        pl.semaphore_signal(barrier, inc=1, device_id={'tp': (z + k) % 4})
    for k in range(1, 8):
        pl.semaphore_signal(barrier, inc=1, device_id={'dp': (d + k) % 8})

    x_all = hid_ref[...].astype(F32)
    g_all = x_all * lax.rsqrt(jnp.mean(x_all * x_all, axis=0, keepdims=True) + NORM_EPS) * (1.0 + w_ref[...])
    gt_ref[...] = g_all.astype(BF16)
    g_scr[...] = jnp.transpose(g_all).astype(BF16)
    s_acc, m_acc, t_acc = wgt, l2s, mtx
    s_acc[...] = jnp.zeros_like(s_acc)
    t_acc[...] = jnp.zeros_like(t_acc)
    m_acc[...] = jnp.full_like(m_acc, -jnp.inf)
    cnt_own[...] = jnp.full((8, 128), jnp.sum(mask_ref[...].astype(F32)), F32)
    dg_ref[...] = jnp.zeros_like(dg_ref)
    kl_acc[...] = jnp.zeros_like(kl_acc)
    dw_acc[...] = jnp.zeros_like(dw_acc)

    def sums(i, three):
        for cp in fetch_tea(i):
            cp.wait()

        @pl.when(i + 2 < NCH)
        def _():
            for cp in fetch_tea(i + 2):
                cp.start()

        @pl.when(i >= 3)
        def _():
            put_th(i - 3).wait()

        tb = TB1
        for blk in range(TOK // tb):
            raw = jnp.dot(g_scr[blk * tb:(blk + 1) * tb, :], emb_buf[three], preferred_element_type=F32)
            for sub in range(tb // RG):
                rows = slice(blk * tb + sub * RG, blk * tb + (sub + 1) * RG)
                th = jnp.tanh(raw[sub * RG:(sub + 1) * RG, :] * (1.0 / SOFT_CAP))
                th_buf[three, rows, :] = th
                s_acc[rows, :] += tree(jnp.add, lane_tiles(jnp.exp2(th * CAP2 - CAP2)))
                tea = lane_tiles(tea_buf[three, rows, :].astype(F32))
                old = m_acc[rows, :]
                new = jnp.maximum(old, tree(jnp.maximum, tea))
                m_acc[rows, :] = new
                t_acc[rows, :] = t_acc[rows, :] * jnp.exp2((old - new) * LOG2E) + tree(
                    jnp.add, [jnp.exp2((part - new) * LOG2E) for part in tea])
        put_th(i).start()

    def sums3(t, carry):
        for three in range(3):
            sums(3 * t + three, three)
        return carry

    lax.fori_loop(0, NCH // 3, sums3, 0)
    for k in range(3):
        put_th(NCH - 3 + k).wait()
    start_fetch(0)
    start_fetch(1)
    s_row = jnp.sum(jnp.transpose(s_acc[...]), axis=0, keepdims=True)
    m_t = jnp.transpose(m_acc[...])
    m_row = jnp.max(m_t, axis=0, keepdims=True)
    t_row = jnp.sum(jnp.transpose(t_acc[...]) * jnp.exp2((m_t - m_row) * LOG2E), axis=0, keepdims=True)
    st_ref[...] = jnp.concatenate([s_row, m_row, t_row, jnp.zeros((5, TOK), F32)], axis=0)
    pl.semaphore_wait(barrier, 10)

    def st_copy(k):
        return pltpu.make_async_remote_copy(
            src_ref=st_ref, dst_ref=st_in.at[k], send_sem=st_send.at[k], recv_sem=st_recv.at[k],
            device_id={'tp': (z + k) % 4})

    def cnt_copy(k):
        return pltpu.make_async_remote_copy(
            src_ref=cnt_own, dst_ref=cnt_in.at[k], send_sem=cnt_send.at[k], recv_sem=cnt_recv.at[k],
            device_id={'dp': (d + k) % 8})

    for k in range(1, 4):
        st_copy(k).start()
    for k in range(1, 8):
        cnt_copy(k).start()
    for k in range(1, 4):
        st_copy(k).wait_recv()
    for k in range(1, 8):
        cnt_copy(k).wait_recv()

    stats = [st_ref[...]] + [st_in[k] for k in range(1, 4)]
    s_tot = tree(jnp.add, [st[0:1, :] for st in stats])
    m_tot = tree(jnp.maximum, [st[1:2, :] for st in stats])
    t_tot = tree(jnp.add, [st[2:3, :] * jnp.exp2((st[1:2, :] - m_tot) * LOG2E) for st in stats])
    count = cnt_own[0:1, :]
    for k in range(1, 8):
        count = count + cnt_in[k][0:1, :]
    w_row = mask_ref[...].astype(F32) / jnp.concatenate([count] * (TOK // 128), axis=1)
    l2s_row = jnp.log2(s_tot) + CAP2
    l2t_row = jnp.log2(t_tot)

    def to_rows(row):
        return jnp.transpose(jnp.broadcast_to(row, (128, TOK)))

    wgt[...] = to_rows(w_row)
    l2s[...] = to_rows(l2s_row)
    mtx[...] = to_rows(m_tot)
    l2t[...] = to_rows(l2t_row)
    lse_part = w_row * ((l2s_row - l2t_row) * LN2 - m_tot)
    lse_sum = jnp.where(z == 0, jnp.sum(lse_part), 0.0)

    def elementwise(i, dr_ref, lo, hi):
        slot = i % 3
        for sub in range(lo, hi):
            rows = slice(sub * RG, (sub + 1) * RG)
            w_b, ls_b, m_b, lt_b = wgt[rows, :], l2s[rows, :], mtx[rows, :], l2t[rows, :]
            kl = []
            for q in range(CW // 128):
                cols = slice(q * 128, (q + 1) * 128)
                th = th_buf[slot, rows, cols]
                tea = tea_buf[slot, rows, cols].astype(F32)
                p_s = jnp.exp2(th * CAP2 - ls_b)
                p_t = jnp.exp2((tea - m_b) * LOG2E - lt_b)
                kl.append(p_t * (tea - SOFT_CAP * th))
                dr_ref[rows, cols] = ((p_s - p_t) * w_b * (1.0 - th * th)).astype(BF16)
            kl_acc[rows, :] += tree(jnp.add, kl)

    def products(i, pp_ref, k):
        rows = slice(k * TB2, (k + 1) * TB2)
        for col in range(rows.start, rows.stop, 256):
            cols = slice(col, col + 256)
            dg_ref[:, cols] += lax.dot_general(emb_buf[i % 3], dr[cols, :], NT, preferred_element_type=F32)
        for half in range(2):
            cols = slice(half * HALF, (half + 1) * HALF)
            part = jnp.dot(gt_ref[:, rows], dr[rows, cols], preferred_element_type=F32)
            for grp in range(8):
                at = (grp % 2, grp // 4, (grp // 2) % 2, slice(None), cols)
                piece = part[grp * GRP:(grp + 1) * GRP, :]
                pp_ref[at] = piece if k == 0 else pp_ref[at] + piece

    def whole(i, pp_ref):
        n = TOK // TB2
        for k in range(n):
            elementwise(i, dr, nsub * k // n, nsub * (k + 1) // n)
            products(i, pp_ref, k)

    def s1_copy(c, pp_ref):
        return pltpu.make_async_remote_copy(
            src_ref=pp_ref.at[1 - core], dst_ref=r1.at[c], send_sem=s1_send.at[c], recv_sem=s1_recv.at[c],
            device_id={'dp': partner})

    def s2_copies(c):
        return (
            pltpu.make_async_remote_copy(
                src_ref=r1.at[c, :, 1 - xx, :, pl.ds(0, HALF)], dst_ref=r2a.at[c],
                send_sem=s2_send.at[0, c], recv_sem=s2_recv.at[0, c], device_id={'dp': xnbr}),
            pltpu.make_async_remote_copy(
                src_ref=r1.at[c, 1 - yy, :, :, pl.ds(HALF, HALF)], dst_ref=r2b.at[c],
                send_sem=s2_send.at[1, c], recv_sem=s2_recv.at[1, c], device_id={'dp': ynbr}),
        )

    def s3_copies(c):
        return (
            pltpu.make_async_remote_copy(
                src_ref=r2a.at[c, 1 - yy], dst_ref=r3a.at[c],
                send_sem=s3_send.at[0, c], recv_sem=s3_recv.at[0, c], device_id={'dp': ynbr}),
            pltpu.make_async_remote_copy(
                src_ref=r2b.at[c, 1 - xx], dst_ref=r3b.at[c],
                send_sem=s3_send.at[1, c], recv_sem=s3_recv.at[1, c], device_id={'dp': xnbr}),
        )

    def stage1(c, pp_ref):
        s1_copy(c, pp_ref).wait_recv()
        for q in range(4):
            r1[c, q // 2, q % 2] += pp_ref[core, q // 2, q % 2]

    def stage2(c):
        for cp in s2_copies(c):
            cp.start()

    def stage3(c):
        first, second = s2_copies(c)
        first.wait_recv()
        for q in range(2):
            r2a[c, q] += r1[c, q, xx, :, 0:HALF]
        second.wait_recv()
        for q in range(2):
            r2b[c, q] += r1[c, yy, q, :, HALF:CW]
        for cp in s3_copies(c):
            cp.start()

    def stage4(c):
        first, second = s3_copies(c)
        base = pl.multiple_of(c * CW, CW)
        first.wait_recv()
        de_ref[:, pl.ds(base, HALF)] = r2a[c, yy] + r3a[c]
        second.wait_recv()
        de_ref[:, pl.ds(pl.multiple_of(base + HALF, HALF), HALF)] = r2b[c, xx] + r3b[c]

    nsub = TOK // RG

    def wait_in(i):
        for cp in fetch(i):
            cp.wait()

    def tick(t):
        stage2(t + 2)

        @pl.when(t >= 1)
        def _():
            stage3(t - 1)

        @pl.when(t >= 4)
        def _():
            stage4(t - 4)

    wait_in(0)
    start_fetch(2)
    whole(0, pp0)
    s1_copy(0, pp0).start()

    def pair(t, carry):
        for par, (pp_new, pp_old) in enumerate(((pp1, pp0), (pp0, pp1))):
            i = 1 + 2 * t + par
            wait_in(i)

            @pl.when(i + 2 < NCH)
            def _():
                start_fetch(i + 2)

            @pl.when(i >= 2)
            def _():
                s1_copy(i - 2, pp_new).wait_send()

            whole(i, pp_new)
            s1_copy(i, pp_new).start()
            stage1(i - 1, pp_old)
            if par == 0:
                @pl.when(t == 0)
                def _():
                    stage2(0)

                @pl.when(t > 0)
                def _():
                    tick(t - 1)
            else:
                @pl.when(t == 0)
                def _():
                    stage2(1)
        return carry

    npair = (NCH - 2) // 2
    lax.fori_loop(0, npair, pair, 0)
    wait_in(NCH - 1)
    s1_copy(NCH - 3, pp1).wait_send()
    whole(NCH - 1, pp1)
    s1_copy(NCH - 1, pp1).start()
    stage1(NCH - 2, pp0)
    tick(npair - 1)

    def where_of(h):
        pos = z if h == 0 else 3 - z
        up = z + 1 if h == 0 else z - 1
        down = z - 1 if h == 0 else z + 1
        return pos, up, down

    def lanes(h, b):
        lo = h * 512 + b * 128
        return slice(lo, lo + 128)

    def ar_first(h, b):
        pos, up, _ = where_of(h)
        idx = 4 * h + b
        return pltpu.make_async_remote_copy(
            src_ref=dg_ref.at[:, pl.ds(h * 512 + b * 128, 128)], dst_ref=ar_in.at[idx],
            send_sem=ar_send.at[idx], recv_sem=ar_recv.at[idx], device_id={'tp': up})

    def ar_next(h, b):
        pos, up, _ = where_of(h)
        idx = 4 * h + b
        return pltpu.make_async_remote_copy(
            src_ref=ar_in.at[idx], dst_ref=ar_in.at[idx],
            send_sem=ar_send.at[idx], recv_sem=ar_recv.at[idx], device_id={'tp': up})

    def bc_copy(h, b):
        _, _, down = where_of(h)
        idx = 4 * h + b
        part = dh_f.at[:, pl.ds(h * 512 + b * 128, 128)]
        return pltpu.make_async_remote_copy(
            src_ref=part, dst_ref=part,
            send_sem=bc_send.at[idx], recv_sem=bc_recv.at[idx], device_id={'tp': down})

    for b in range(4):
        for h in range(2):
            @pl.when(where_of(h)[0] == 0)
            def _():
                ar_first(h, b).start()

    def add_on(h, b):
        idx = 4 * h + b
        ar_next(h, b).wait_recv()
        ar_in[idx] += dg_ref[:, lanes(h, b)]
        ar_next(h, b).start()

    def finish(h, b):
        ar_next(h, b).wait_recv()
        dg = ar_in[4 * h + b] + dg_ref[:, lanes(h, b)]
        x = hid_ref[:, lanes(h, b)].astype(F32)
        inv = lax.rsqrt(jnp.mean(x * x, axis=0, keepdims=True) + NORM_EPS)
        dw_acc[...] += dg * (x * inv)
        du = dg * (1.0 + w_ref[...])
        inner = jnp.sum(du * x, axis=0, keepdims=True)
        dh_f[:, lanes(h, b)] = du * inv - x * (inv * inv * inv * inner * (1.0 / D))
        bc_copy(h, b).start()

    def spread(h, b, pos):
        bc_copy(h, b).wait_recv()
        if pos > 0:
            bc_copy(h, b).start()

    def slot(s):
        for pos in (1, 2, 3):
            b = s - (pos - 1)
            if 0 <= b < 4:
                for h in range(2):
                    @pl.when(where_of(h)[0] == pos)
                    def _():
                        if pos < 3:
                            add_on(h, b)
                        else:
                            finish(h, b)
        for pos in (2, 1, 0):
            b = s - 4 - (2 - pos)
            if 0 <= b < 4:
                for h in range(2):
                    @pl.when(where_of(h)[0] == pos)
                    def _():
                        spread(h, b, pos)

    def wsum(k, carry):
        rows = pl.ds(pl.multiple_of(k * 8, 8), 8)
        return carry + wgt[rows, :] * kl_acc[rows, :]

    def small_copy(k, over):
        mine, size, buf, send, recv = (
            (d, 8, sm_dp, smd_send, smd_recv) if over == 'dp' else (z, 4, sm_tp, smt_send, smt_recv))
        peer = (mine + k) % size
        return pltpu.make_async_remote_copy(
            src_ref=buf.at[mine], dst_ref=buf.at[mine], send_sem=send.at[k], recv_sem=recv.at[mine],
            device_id={over: peer})

    def small_wait(k, over):
        mine, size, buf, send, recv = (
            (d, 8, sm_dp, smd_send, smd_recv) if over == 'dp' else (z, 4, sm_tp, smt_send, smt_recv))
        peer = (mine + k) % size
        pltpu.make_async_remote_copy(
            src_ref=buf.at[peer], dst_ref=buf.at[peer], send_sem=send.at[k], recv_sem=recv.at[peer],
            device_id={over: peer}).wait_recv()

    def small_dp():
        kl_tile = lax.fori_loop(0, TOK // 8, wsum, jnp.zeros((8, 128), F32))
        loss = jnp.sum(kl_tile) + lse_sum
        dw_row = jnp.sum(jnp.transpose(dw_acc[...]), axis=0, keepdims=True)
        sm_dp[d] = jnp.concatenate([dw_row, jnp.full((1, D), loss, F32), jnp.zeros((6, D), F32)], axis=0)
        for k in range(1, 8):
            small_copy(k, 'dp').start()

    def small_tp():
        for k in range(1, 8):
            small_wait(k, 'dp')
        sm_tp[z] = tree(jnp.add, [sm_dp[k] for k in range(8)])
        for k in range(1, 4):
            small_copy(k, 'tp').start()

    def small_end():
        for k in range(1, 4):
            small_wait(k, 'tp')
        small_ref[...] = tree(jnp.add, [sm_tp[k] for k in range(4)])

    def ticks(lo, hi):
        def body(t, carry):
            tick(t)
            return carry
        lax.fori_loop(lo, hi, body, 0)

    stage1(NCH - 1, pp1)
    t0 = npair
    for n, cuts in enumerate((0, 1, 2, 4, 5, 7, 8, 10)):
        ticks(t0 + cuts, t0 + (1, 2, 4, 5, 7, 8, 10, NCH - 2 - t0)[n])
        slot(n)
        if n == 6:
            small_dp()
    stage3(NCH - 3)
    stage4(NCH - 6)
    slot(8)
    stage3(NCH - 2)
    stage4(NCH - 5)
    small_tp()
    stage3(NCH - 1)
    stage4(NCH - 4)
    slot(9)
    dh_ref[...] = dh_f[...].astype(BF16)
    stage4(NCH - 3)
    stage4(NCH - 2)
    stage4(NCH - 1)
    small_end()

    for k in range(1, 4):
        st_copy(k).wait_send()
    for k in range(1, 8):
        cnt_copy(k).wait_send()
    s1_copy(NCH - 2, pp0).wait_send()
    s1_copy(NCH - 1, pp1).wait_send()

    def drain(c):
        for cp in s2_copies(c) + s3_copies(c):
            cp.wait_send()

    def drain_body(c, carry):
        drain(c)
        return carry

    lax.fori_loop(0, NCH, drain_body, 0)
    for k in range(1, 8):
        small_copy(k, 'dp').wait_send()
    for k in range(1, 4):
        small_copy(k, 'tp').wait_send()
    for h in range(2):
        pos = where_of(h)[0]
        for b in range(4):
            @pl.when(pos < 3)
            def _():
                ar_next(h, b).wait_send()

            @pl.when(pos > 0)
            def _():
                bc_copy(h, b).wait_send()


def one_pass(teach, emb_t, hid_t, w_col, mask_row):
    vmem = pl.BlockSpec(memory_space=pltpu.VMEM)
    hbm = pl.BlockSpec(memory_space=pl.ANY)
    dma = pltpu.SemaphoreType.DMA
    return pl.pallas_call(
        grad_kernel,
        out_shape=(
            jax.ShapeDtypeStruct((TOK, VLOC), F32),
            jax.ShapeDtypeStruct((GRP, VLOC), F32),
            jax.ShapeDtypeStruct((D, TOK), BF16),
            jax.ShapeDtypeStruct((8, D), F32),
        ),
        in_specs=[hbm] * 2 + [vmem] * 3,
        out_specs=(hbm,) + (vmem,) * 3,
        scratch_shapes=[
            pltpu.VMEM((TOK, D), BF16),
            pltpu.VMEM((D, TOK), BF16),
            pltpu.VMEM((8, TOK), F32),
            dma((3,)),
            pltpu.VMEM((3, TOK, CW), F32),
            pltpu.VMEM((3, TOK, CW), BF16),
            pltpu.VMEM((3, D, CW), BF16),
            pltpu.VMEM((TOK, CW), BF16),
            pltpu.VMEM((2, 2, 2, GRP, CW), F32),
            pltpu.VMEM((2, 2, 2, GRP, CW), F32),
            pltpu.VMEM((NCH, 2, 2, GRP, CW), F32),
            pltpu.VMEM((NCH, 2, GRP, HALF), F32),
            pltpu.VMEM((NCH, 2, GRP, HALF), F32),
            pltpu.VMEM((NCH, GRP, HALF), F32),
            pltpu.VMEM((NCH, GRP, HALF), F32),
            pltpu.VMEM((D, TOK), F32),
            pltpu.VMEM((8, D, 128), F32),
            pltpu.VMEM((D, TOK), F32),
            pltpu.VMEM((4, 8, TOK), F32),
            pltpu.VMEM((8, 8, 128), F32),
            pltpu.VMEM((8, 128), F32),
            pltpu.VMEM((D, 128), F32),
            pltpu.VMEM((8, 8, D), F32),
            pltpu.VMEM((4, 8, D), F32),
        ] + [pltpu.VMEM((TOK, 128), F32)] * 5 + [
            dma((3, 3)), dma((4,)), dma((4,)), dma((8,)), dma((8,)),
            dma((NCH,)), dma((NCH,)), dma((2, NCH)), dma((2, NCH)), dma((2, NCH)), dma((2, NCH)),
            dma((8,)), dma((8,)), dma((8,)), dma((8,)),
            dma((8,)), dma((8,)), dma((4,)), dma((4,)),
        ],
        compiler_params=pltpu.CompilerParams(
            collective_id=0, has_side_effects=True, vmem_limit_bytes=67_000_000),
        cost_estimate=pl.CostEstimate(
            flops=6 * TOK * VLOC * D, bytes_accessed=190_000_000, transcendentals=5 * TOK * VLOC),
    )(teach, emb_t, hid_t, w_col, mask_row)


def solution(mesh):
    def device_fn(hid_loc, norm_w, emb_loc, teach_loc, mask_loc):
        hid_t = hid_loc.T
        emb_t = emb_loc.T
        w_col = norm_w.astype(F32).reshape(D, 1)
        mask_row = mask_loc.reshape(1, TOK)
        _, de_t, dh_t, small = one_pass(teach_loc, emb_t, hid_t, w_col, mask_row)
        return small[1, 0], dh_t.T, de_t.T, small[0]

    return jax.shard_map(device_fn, mesh=mesh, in_specs=(P('dp', None), P(None), P('tp', None), P('dp', 'tp'), P('dp')), out_specs=(P(), P('dp', None), P('tp', 'dp'), P(None)), check_vma=False)
```

```python
import jax
import jax.numpy as jnp
from jax import lax
from jax.experimental import pallas as pl
from jax.experimental.pallas import tpu as pltpu
from jax.sharding import PartitionSpec as P

SOFT_CAP = 30.0
NORM_EPS = 1e-6
LOG2E = 1.4426950408889634
LN2 = 0.6931471805599453
CAP2 = SOFT_CAP * LOG2E
D = 576
GRP = 72
TOK = 1024
VLOC = 12288
CW = 512
HALF = CW // 2
NCH = VLOC // CW
RG = 32
TB1 = 128
TB2 = 512
F32 = jnp.float32
BF16 = jnp.bfloat16
NT = (((1,), (1,)), ((), ()))


def lane_tiles(arr):
    return [arr[:, k * 128:(k + 1) * 128] for k in range(arr.shape[1] // 128)]


def tree(op, parts):
    while len(parts) > 1:
        parts = [op(parts[k], parts[k + 1]) if k + 1 < len(parts) else parts[k] for k in range(0, len(parts), 2)]
    return parts[0]


def grad_kernel(tea_hbm, emb_hbm, hid_ref, w_ref, mask_ref,
                th_hbm, de_ref, dh_ref, small_ref,
                g_scr, gt_ref, st_ref, out_sem,
                th_buf, tea_buf, emb_buf, dr, pp0, pp1, r1, r2a, r2b, r3a, r3b,
                dg_ref, ar_in, dh_f, st_in, cnt_in, cnt_own, dw_acc, sm_dp, sm_tp, wgt, l2s, mtx, l2t, kl_acc,
                in_sem, st_send, st_recv, cnt_send, cnt_recv,
                s1_send, s1_recv, s2_send, s2_recv, s3_send, s3_recv,
                ar_send, ar_recv, bc_send, bc_recv, smd_send, smd_recv, smt_send, smt_recv):
    z = lax.axis_index('tp')
    d = lax.axis_index('dp')
    core = d % 2
    xx = (d // 2) % 2
    yy = d // 4
    partner = d + 1 - 2 * core
    xnbr = d + 2 - 4 * xx
    ynbr = d + 4 - 8 * yy

    def fetch(i):
        cols = pl.ds(pl.multiple_of(i * CW, CW), CW)
        three = i % 3
        return (
            pltpu.make_async_copy(th_hbm.at[:, cols], th_buf.at[three], in_sem.at[0, three]),
            pltpu.make_async_copy(tea_hbm.at[:, cols], tea_buf.at[three], in_sem.at[1, three]),
            pltpu.make_async_copy(emb_hbm.at[:, cols], emb_buf.at[three], in_sem.at[2, three]),
        )

    def start_fetch(i):
        for cp in fetch(i):
            cp.start()

    def fetch_tea(i):
        cols = pl.ds(pl.multiple_of(i * CW, CW), CW)
        three = i % 3
        return (
            pltpu.make_async_copy(tea_hbm.at[:, cols], tea_buf.at[three], in_sem.at[1, three]),
            pltpu.make_async_copy(emb_hbm.at[:, cols], emb_buf.at[three], in_sem.at[2, three]),
        )

    def put_th(i):
        cols = pl.ds(pl.multiple_of(i * CW, CW), CW)
        three = i % 3
        return pltpu.make_async_copy(th_buf.at[three], th_hbm.at[:, cols], out_sem.at[three])

    for k in range(2):
        for cp in fetch_tea(k):
            cp.start()

    barrier = pltpu.get_barrier_semaphore()
    for k in range(1, 4):
        pl.semaphore_signal(barrier, inc=1, device_id={'tp': (z + k) % 4})
    for k in range(1, 8):
        pl.semaphore_signal(barrier, inc=1, device_id={'dp': (d + k) % 8})

    x_all = hid_ref[...].astype(F32)
    g_all = x_all * lax.rsqrt(jnp.mean(x_all * x_all, axis=0, keepdims=True) + NORM_EPS) * (1.0 + w_ref[...])
    gt_ref[...] = g_all.astype(BF16)
    g_scr[...] = jnp.transpose(g_all).astype(BF16)
    s_acc, m_acc, t_acc = wgt, l2s, mtx
    s_acc[...] = jnp.zeros_like(s_acc)
    t_acc[...] = jnp.zeros_like(t_acc)
    m_acc[...] = jnp.full_like(m_acc, -jnp.inf)
    cnt_own[...] = jnp.full((8, 128), jnp.sum(mask_ref[...].astype(F32)), F32)
    dg_ref[...] = jnp.zeros_like(dg_ref)
    kl_acc[...] = jnp.zeros_like(kl_acc)
    dw_acc[...] = jnp.zeros_like(dw_acc)

    def sums(i, three):
        for cp in fetch_tea(i):
            cp.wait()

        @pl.when(i + 2 < NCH)
        def _():
            for cp in fetch_tea(i + 2):
                cp.start()

        @pl.when(i >= 3)
        def _():
            put_th(i - 3).wait()

        tb = TB1
        for blk in range(TOK // tb):
            raw = jnp.dot(g_scr[blk * tb:(blk + 1) * tb, :], emb_buf[three], preferred_element_type=F32)
            for sub in range(tb // RG):
                rows = slice(blk * tb + sub * RG, blk * tb + (sub + 1) * RG)
                th = jnp.tanh(raw[sub * RG:(sub + 1) * RG, :] * (1.0 / SOFT_CAP))
                th_buf[three, rows, :] = th
                s_acc[rows, :] += tree(jnp.add, lane_tiles(jnp.exp2(th * CAP2)))
                tea = lane_tiles(tea_buf[three, rows, :].astype(F32))
                old = m_acc[rows, :]
                new = jnp.maximum(old, tree(jnp.maximum, tea))
                m_acc[rows, :] = new
                t_acc[rows, :] = t_acc[rows, :] * jnp.exp2((old - new) * LOG2E) + tree(
                    jnp.add, [jnp.exp2((part - new) * LOG2E) for part in tea])
        put_th(i).start()

    def sums3(t, carry):
        for three in range(3):
            sums(3 * t + three, three)
        return carry

    lax.fori_loop(0, NCH // 3, sums3, 0)
    for k in range(3):
        put_th(NCH - 3 + k).wait()
    start_fetch(0)
    start_fetch(1)
    s_row = jnp.sum(jnp.transpose(s_acc[...]), axis=0, keepdims=True)
    m_t = jnp.transpose(m_acc[...])
    m_row = jnp.max(m_t, axis=0, keepdims=True)
    t_row = jnp.sum(jnp.transpose(t_acc[...]) * jnp.exp2((m_t - m_row) * LOG2E), axis=0, keepdims=True)
    st_ref[...] = jnp.concatenate([s_row, m_row, t_row, jnp.zeros((5, TOK), F32)], axis=0)
    pl.semaphore_wait(barrier, 10)

    def st_copy(k):
        return pltpu.make_async_remote_copy(
            src_ref=st_ref, dst_ref=st_in.at[k], send_sem=st_send.at[k], recv_sem=st_recv.at[k],
            device_id={'tp': (z + k) % 4})

    def cnt_copy(k):
        return pltpu.make_async_remote_copy(
            src_ref=cnt_own, dst_ref=cnt_in.at[k], send_sem=cnt_send.at[k], recv_sem=cnt_recv.at[k],
            device_id={'dp': (d + k) % 8})

    for k in range(1, 4):
        st_copy(k).start()
    for k in range(1, 8):
        cnt_copy(k).start()
    for k in range(1, 4):
        st_copy(k).wait_recv()
    for k in range(1, 8):
        cnt_copy(k).wait_recv()

    stats = [st_ref[...]] + [st_in[k] for k in range(1, 4)]
    s_tot = tree(jnp.add, [st[0:1, :] for st in stats])
    m_tot = tree(jnp.maximum, [st[1:2, :] for st in stats])
    t_tot = tree(jnp.add, [st[2:3, :] * jnp.exp2((st[1:2, :] - m_tot) * LOG2E) for st in stats])
    count = cnt_own[0:1, :]
    for k in range(1, 8):
        count = count + cnt_in[k][0:1, :]
    w_row = mask_ref[...].astype(F32) / jnp.concatenate([count] * (TOK // 128), axis=1)
    l2s_row = jnp.log2(s_tot)
    l2t_row = jnp.log2(t_tot)

    def to_rows(row):
        return jnp.transpose(jnp.broadcast_to(row, (128, TOK)))

    l2w_row = jnp.log2(w_row)
    l2s[...] = to_rows(l2s_row - l2w_row)
    mtx[...] = to_rows(m_tot)
    l2t[...] = to_rows(l2t_row - l2w_row)
    lse_part = w_row * ((l2s_row - l2t_row) * LN2 - m_tot)
    lse_sum = jnp.where(z == 0, jnp.sum(lse_part), 0.0)

    def elementwise(i, dr_ref, lo, hi):
        slot = i % 3
        for sub in range(lo, hi):
            rows = slice(sub * RG, (sub + 1) * RG)
            ls_b, m_b, lt_b = l2s[rows, :], mtx[rows, :], l2t[rows, :]
            kl = []
            for q in range(CW // 128):
                cols = slice(q * 128, (q + 1) * 128)
                th = th_buf[slot, rows, cols]
                tea = tea_buf[slot, rows, cols].astype(F32)
                p_s = jnp.exp2(th * CAP2 - ls_b)
                p_t = jnp.exp2((tea - m_b) * LOG2E - lt_b)
                kl.append(p_t * (tea - SOFT_CAP * th))
                dr_ref[rows, cols] = ((p_s - p_t) * (1.0 - th * th)).astype(BF16)
            kl_acc[rows, :] += tree(jnp.add, kl)

    def products(i, pp_ref, k):
        rows = slice(k * TB2, (k + 1) * TB2)
        for col in range(rows.start, rows.stop, 256):
            cols = slice(col, col + 256)
            dg_ref[:, cols] += lax.dot_general(emb_buf[i % 3], dr[cols, :], NT, preferred_element_type=F32)
        for half in range(2):
            cols = slice(half * HALF, (half + 1) * HALF)
            part = jnp.dot(gt_ref[:, rows], dr[rows, cols], preferred_element_type=F32)
            for grp in range(8):
                at = (grp % 2, grp // 4, (grp // 2) % 2, slice(None), cols)
                piece = part[grp * GRP:(grp + 1) * GRP, :]
                pp_ref[at] = piece if k == 0 else pp_ref[at] + piece

    def whole(i, pp_ref):
        n = TOK // TB2
        for k in range(n):
            elementwise(i, dr, nsub * k // n, nsub * (k + 1) // n)
            products(i, pp_ref, k)

    def s1_copy(c, pp_ref):
        return pltpu.make_async_remote_copy(
            src_ref=pp_ref.at[1 - core], dst_ref=r1.at[c], send_sem=s1_send.at[c], recv_sem=s1_recv.at[c],
            device_id={'dp': partner})

    def s2_copies(c):
        return (
            pltpu.make_async_remote_copy(
                src_ref=r1.at[c, :, 1 - xx, :, pl.ds(0, HALF)], dst_ref=r2a.at[c],
                send_sem=s2_send.at[0, c], recv_sem=s2_recv.at[0, c], device_id={'dp': xnbr}),
            pltpu.make_async_remote_copy(
                src_ref=r1.at[c, 1 - yy, :, :, pl.ds(HALF, HALF)], dst_ref=r2b.at[c],
                send_sem=s2_send.at[1, c], recv_sem=s2_recv.at[1, c], device_id={'dp': ynbr}),
        )

    def s3_copies(c):
        return (
            pltpu.make_async_remote_copy(
                src_ref=r2a.at[c, 1 - yy], dst_ref=r3a.at[c],
                send_sem=s3_send.at[0, c], recv_sem=s3_recv.at[0, c], device_id={'dp': ynbr}),
            pltpu.make_async_remote_copy(
                src_ref=r2b.at[c, 1 - xx], dst_ref=r3b.at[c],
                send_sem=s3_send.at[1, c], recv_sem=s3_recv.at[1, c], device_id={'dp': xnbr}),
        )

    def stage1(c, pp_ref):
        s1_copy(c, pp_ref).wait_recv()
        for q in range(4):
            r1[c, q // 2, q % 2] += pp_ref[core, q // 2, q % 2]

    def stage2(c):
        for cp in s2_copies(c):
            cp.start()

    def stage3(c):
        first, second = s2_copies(c)
        first.wait_recv()
        for q in range(2):
            r2a[c, q] += r1[c, q, xx, :, 0:HALF]
        second.wait_recv()
        for q in range(2):
            r2b[c, q] += r1[c, yy, q, :, HALF:CW]
        for cp in s3_copies(c):
            cp.start()

    def stage4(c):
        first, second = s3_copies(c)
        base = pl.multiple_of(c * CW, CW)
        first.wait_recv()
        de_ref[:, pl.ds(base, HALF)] = r2a[c, yy] + r3a[c]
        second.wait_recv()
        de_ref[:, pl.ds(pl.multiple_of(base + HALF, HALF), HALF)] = r2b[c, xx] + r3b[c]

    nsub = TOK // RG

    def wait_in(i):
        for cp in fetch(i):
            cp.wait()

    def tick(t):
        stage2(t + 2)

        @pl.when(t >= 1)
        def _():
            stage3(t - 1)

        @pl.when(t >= 4)
        def _():
            stage4(t - 4)

    wait_in(0)
    start_fetch(2)
    whole(0, pp0)
    s1_copy(0, pp0).start()

    def pair(t, carry):
        for par, (pp_new, pp_old) in enumerate(((pp1, pp0), (pp0, pp1))):
            i = 1 + 2 * t + par
            wait_in(i)

            @pl.when(i + 2 < NCH)
            def _():
                start_fetch(i + 2)

            @pl.when(i >= 2)
            def _():
                s1_copy(i - 2, pp_new).wait_send()

            whole(i, pp_new)
            s1_copy(i, pp_new).start()
            stage1(i - 1, pp_old)
            if par == 0:
                @pl.when(t == 0)
                def _():
                    stage2(0)

                @pl.when(t > 0)
                def _():
                    tick(t - 1)
            else:
                @pl.when(t == 0)
                def _():
                    stage2(1)
        return carry

    npair = (NCH - 2) // 2
    lax.fori_loop(0, npair, pair, 0)
    wait_in(NCH - 1)
    s1_copy(NCH - 3, pp1).wait_send()
    whole(NCH - 1, pp1)
    s1_copy(NCH - 1, pp1).start()
    stage1(NCH - 2, pp0)
    tick(npair - 1)

    def where_of(h):
        pos = z if h == 0 else 3 - z
        up = z + 1 if h == 0 else z - 1
        down = z - 1 if h == 0 else z + 1
        return pos, up, down

    def lanes(h, b):
        lo = h * 512 + b * 128
        return slice(lo, lo + 128)

    def rows_of(r):
        return pl.ds(r * (D // 2), D // 2)

    def ar_copy(h, b, r, first=False):
        _, up, _ = where_of(h)
        idx = 4 * h + b
        dst = ar_in.at[idx, rows_of(r)]
        src = dg_ref.at[rows_of(r), pl.ds(h * 512 + b * 128, 128)] if first else dst
        return pltpu.make_async_remote_copy(
            src_ref=src, dst_ref=dst,
            send_sem=ar_send.at[2 * idx + r], recv_sem=ar_recv.at[2 * idx + r], device_id={'tp': up})

    def bc_copy(h, b, r):
        _, _, down = where_of(h)
        idx = 4 * h + b
        part = dh_f.at[rows_of(r), pl.ds(h * 512 + b * 128, 128)]
        return pltpu.make_async_remote_copy(
            src_ref=part, dst_ref=part,
            send_sem=bc_send.at[2 * idx + r], recv_sem=bc_recv.at[2 * idx + r], device_id={'tp': down})

    for b in range(4):
        for h in range(2):
            @pl.when(where_of(h)[0] == 0)
            def _():
                for r in range(2):
                    ar_copy(h, b, r, first=True).start()

    def add_on(h, b):
        idx = 4 * h + b
        for r in range(2):
            ar_copy(h, b, r).wait_recv()
            ar_in[idx, rows_of(r)] += dg_ref[rows_of(r), lanes(h, b)]
            ar_copy(h, b, r).start()

    def finish(h, b):
        for r in range(2):
            ar_copy(h, b, r).wait_recv()
        dg = ar_in[4 * h + b] + dg_ref[:, lanes(h, b)]
        x = hid_ref[:, lanes(h, b)].astype(F32)
        inv = lax.rsqrt(jnp.mean(x * x, axis=0, keepdims=True) + NORM_EPS)
        dw_acc[...] += dg * (x * inv)
        du = dg * (1.0 + w_ref[...])
        inner = jnp.sum(du * x, axis=0, keepdims=True)
        dh_f[:, lanes(h, b)] = du * inv - x * (inv * inv * inv * inner * (1.0 / D))
        for r in range(2):
            bc_copy(h, b, r).start()

    def spread(h, b, pos):
        for r in range(2):
            bc_copy(h, b, r).wait_recv()
            if pos > 0:
                bc_copy(h, b, r).start()

    def slot(s):
        for pos in (1, 2, 3):
            b = s - (pos - 1)
            if 0 <= b < 4:
                for h in range(2):
                    @pl.when(where_of(h)[0] == pos)
                    def _():
                        if pos < 3:
                            add_on(h, b)
                        else:
                            finish(h, b)
        for pos in (2, 1, 0):
            b = s - 3 - (2 - pos)
            if 0 <= b < 4:
                for h in range(2):
                    @pl.when(where_of(h)[0] == pos)
                    def _():
                        spread(h, b, pos)

    def wsum(k, carry):
        rows = pl.ds(pl.multiple_of(k * 8, 8), 8)
        return carry + kl_acc[rows, :]

    def small_copy(k, over):
        mine, size, buf, send, recv = (
            (d, 8, sm_dp, smd_send, smd_recv) if over == 'dp' else (z, 4, sm_tp, smt_send, smt_recv))
        peer = (mine + k) % size
        return pltpu.make_async_remote_copy(
            src_ref=buf.at[mine], dst_ref=buf.at[mine], send_sem=send.at[k], recv_sem=recv.at[mine],
            device_id={over: peer})

    def small_wait(k, over):
        mine, size, buf, send, recv = (
            (d, 8, sm_dp, smd_send, smd_recv) if over == 'dp' else (z, 4, sm_tp, smt_send, smt_recv))
        peer = (mine + k) % size
        pltpu.make_async_remote_copy(
            src_ref=buf.at[peer], dst_ref=buf.at[peer], send_sem=send.at[k], recv_sem=recv.at[peer],
            device_id={over: peer}).wait_recv()

    def small_dp():
        kl_tile = lax.fori_loop(0, TOK // 8, wsum, jnp.zeros((8, 128), F32))
        loss = jnp.sum(kl_tile) + lse_sum
        dw_row = jnp.sum(jnp.transpose(dw_acc[...]), axis=0, keepdims=True)
        sm_dp[d] = jnp.concatenate([dw_row, jnp.full((1, D), loss, F32), jnp.zeros((6, D), F32)], axis=0)
        for k in range(1, 8):
            small_copy(k, 'dp').start()

    def small_tp():
        for k in range(1, 8):
            small_wait(k, 'dp')
        sm_tp[z] = tree(jnp.add, [sm_dp[k] for k in range(8)])
        for k in range(1, 4):
            small_copy(k, 'tp').start()

    def small_end():
        for k in range(1, 4):
            small_wait(k, 'tp')
        small_ref[...] = tree(jnp.add, [sm_tp[k] for k in range(4)])

    def ticks(lo, hi):
        def body(t, carry):
            tick(t)
            return carry
        lax.fori_loop(lo, hi, body, 0)

    stage1(NCH - 1, pp1)
    t0 = npair
    before = (0, 1, 2, 3, 5, 6, 8, 9, NCH - 2 - t0)
    for n in range(8):
        ticks(t0 + before[n], t0 + before[n + 1])
        slot(n)
        if n == 5:
            small_dp()
    stage3(NCH - 3)
    stage4(NCH - 6)
    slot(8)
    stage3(NCH - 2)
    stage4(NCH - 5)
    small_tp()
    stage3(NCH - 1)
    stage4(NCH - 4)
    dh_ref[...] = dh_f[...].astype(BF16)
    stage4(NCH - 3)
    stage4(NCH - 2)
    stage4(NCH - 1)
    small_end()

    for k in range(1, 4):
        st_copy(k).wait_send()
    for k in range(1, 8):
        cnt_copy(k).wait_send()
    s1_copy(NCH - 2, pp0).wait_send()
    s1_copy(NCH - 1, pp1).wait_send()

    def drain(c):
        for cp in s2_copies(c) + s3_copies(c):
            cp.wait_send()

    def drain_body(c, carry):
        drain(c)
        return carry

    lax.fori_loop(0, NCH, drain_body, 0)
    for k in range(1, 8):
        small_copy(k, 'dp').wait_send()
    for k in range(1, 4):
        small_copy(k, 'tp').wait_send()
    for h in range(2):
        pos = where_of(h)[0]
        for b in range(4):
            for r in range(2):
                @pl.when(pos < 3)
                def _():
                    ar_copy(h, b, r).wait_send()

                @pl.when(pos > 0)
                def _():
                    bc_copy(h, b, r).wait_send()


def one_pass(teach, emb_t, hid_t, w_col, mask_row):
    vmem = pl.BlockSpec(memory_space=pltpu.VMEM)
    hbm = pl.BlockSpec(memory_space=pl.ANY)
    dma = pltpu.SemaphoreType.DMA
    return pl.pallas_call(
        grad_kernel,
        out_shape=(
            jax.ShapeDtypeStruct((TOK, VLOC), F32),
            jax.ShapeDtypeStruct((GRP, VLOC), F32),
            jax.ShapeDtypeStruct((D, TOK), BF16),
            jax.ShapeDtypeStruct((8, D), F32),
        ),
        in_specs=[hbm] * 2 + [vmem] * 3,
        out_specs=(hbm,) + (vmem,) * 3,
        scratch_shapes=[
            pltpu.VMEM((TOK, D), BF16),
            pltpu.VMEM((D, TOK), BF16),
            pltpu.VMEM((8, TOK), F32),
            dma((3,)),
            pltpu.VMEM((3, TOK, CW), F32),
            pltpu.VMEM((3, TOK, CW), BF16),
            pltpu.VMEM((3, D, CW), BF16),
            pltpu.VMEM((TOK, CW), BF16),
            pltpu.VMEM((2, 2, 2, GRP, CW), F32),
            pltpu.VMEM((2, 2, 2, GRP, CW), F32),
            pltpu.VMEM((NCH, 2, 2, GRP, CW), F32),
            pltpu.VMEM((NCH, 2, GRP, HALF), F32),
            pltpu.VMEM((NCH, 2, GRP, HALF), F32),
            pltpu.VMEM((NCH, GRP, HALF), F32),
            pltpu.VMEM((NCH, GRP, HALF), F32),
            pltpu.VMEM((D, TOK), F32),
            pltpu.VMEM((8, D, 128), F32),
            pltpu.VMEM((D, TOK), F32),
            pltpu.VMEM((4, 8, TOK), F32),
            pltpu.VMEM((8, 8, 128), F32),
            pltpu.VMEM((8, 128), F32),
            pltpu.VMEM((D, 128), F32),
            pltpu.VMEM((8, 8, D), F32),
            pltpu.VMEM((4, 8, D), F32),
        ] + [pltpu.VMEM((TOK, 128), F32)] * 5 + [
            dma((3, 3)), dma((4,)), dma((4,)), dma((8,)), dma((8,)),
            dma((NCH,)), dma((NCH,)), dma((2, NCH)), dma((2, NCH)), dma((2, NCH)), dma((2, NCH)),
            dma((16,)), dma((16,)), dma((16,)), dma((16,)),
            dma((8,)), dma((8,)), dma((4,)), dma((4,)),
        ],
        compiler_params=pltpu.CompilerParams(
            collective_id=0, has_side_effects=True, vmem_limit_bytes=67_000_000),
        cost_estimate=pl.CostEstimate(
            flops=6 * TOK * VLOC * D, bytes_accessed=190_000_000, transcendentals=5 * TOK * VLOC),
    )(teach, emb_t, hid_t, w_col, mask_row)


def out_kernel(de_in, dh_in, de_out, dh_out, de_buf, dh_buf, sem_in, sem_out):
    n = 6
    wide = VLOC // n
    pieces = [(dh_in, dh_buf, dh_out)] + [
        (de_in.at[:, pl.ds(k * wide, wide)], de_buf.at[k], de_out.at[:, pl.ds(k * wide, wide)]) for k in range(n)]
    ins = [pltpu.make_async_copy(src, buf, sem_in.at[k]) for k, (src, buf, _) in enumerate(pieces)]
    outs = [pltpu.make_async_copy(buf, dst, sem_out.at[k]) for k, (_, buf, dst) in enumerate(pieces)]
    for cp in ins:
        cp.start()
    for arrive, leave in zip(ins, outs):
        arrive.wait()
        leave.start()
    for cp in outs:
        cp.wait()


def hand_over(de_t, dh_t):
    hbm = pl.BlockSpec(memory_space=pl.ANY)
    return pl.pallas_call(
        out_kernel,
        out_shape=(jax.ShapeDtypeStruct((GRP, VLOC), F32), jax.ShapeDtypeStruct((D, TOK), BF16)),
        in_specs=[hbm] * 2,
        out_specs=(hbm,) * 2,
        scratch_shapes=[
            pltpu.VMEM((6, GRP, VLOC // 6), F32), pltpu.VMEM((D, TOK), BF16),
            pltpu.SemaphoreType.DMA((7,)), pltpu.SemaphoreType.DMA((7,))],
        compiler_params=pltpu.CompilerParams(vmem_limit_bytes=60 * 1024 * 1024),
    )(de_t, dh_t)


def solution(mesh):
    def device_fn(hid_loc, norm_w, emb_loc, teach_loc, mask_loc):
        hid_t = hid_loc.T
        emb_t = emb_loc.T
        w_col = norm_w.astype(F32).reshape(D, 1)
        mask_row = mask_loc.reshape(1, TOK)
        _, de_t, dh_t, small = one_pass(teach_loc, emb_t, hid_t, w_col, mask_row)
        de_t, dh_t = hand_over(de_t, dh_t)
        return small[1, 0], dh_t.T, de_t.T, small[0]

    return jax.shard_map(device_fn, mesh=mesh, in_specs=(P('dp', None), P(None), P('tp', None), P('dp', 'tp'), P('dp')), out_specs=(P(), P('dp', None), P('tp', 'dp'), P(None)), check_vma=False)
```
